8 devices in a mesh: dp: 1 (over z), tp: 8 (over x, y, core).
Axes of the slice: x: 2, y: 2, z: 1, core: 2. Of those that a mesh axis runs over, the one named last changes fastest.
Arguments:
- x: bfloat16 [1, 2048, 4096], P('dp', 'tp')
- dy: bfloat16 [1, 2048, 4096], P('dp', 'tp')
- wq: bfloat16 [4096, 4096], P(None, 'tp')
- wk: bfloat16 [4096, 1024], P(None, 'tp')
- wv: bfloat16 [4096, 1024], P(None, 'tp')
- wo: bfloat16 [4096, 4096], P('tp')
- w_gate: bfloat16 [4096, 12288], P(None, 'tp')
- w_up: bfloat16 [4096, 12288], P(None, 'tp')
- w_down: bfloat16 [12288, 4096], P('tp')
Outputs:
- output 1: bfloat16 [1, 2048, 4096], P('dp', 'tp')
- output 2: bfloat16 [4096, 4096], P('dp', 'tp')
- output 3: bfloat16 [4096, 1024], P('dp', 'tp')
- output 4: bfloat16 [4096, 1024], P('dp', 'tp')
- output 5: bfloat16 [4096, 4096], P(('dp', 'tp'))
- output 6: bfloat16 [4096, 12288], P('dp', 'tp')
- output 7: bfloat16 [4096, 12288], P('dp', 'tp')
- output 8: bfloat16 [12288, 4096], P(('dp', 'tp'))
All inputs are finite; a program needn't handle non-finite values.
Results may differ from the reference program's by a relative error of at most 0.024.
Values are sent between devices in bfloat16 or wider.
A program may use at most 2 GiB of HBM per device.

```python
import jax
import jax.numpy as jnp
from jax import lax

SEQUENCES = 1
TOKENS = 2048
D = 4096
HEADS = 32
KV_HEADS = 8
HEAD = 128
FF = 12288
THETA = 10000
NAMES = ("wq", "wk", "wv", "wo", "w_gate", "w_up", "w_down")
SHAPES = {
    "wq": (D, HEADS * HEAD),
    "wk": (D, KV_HEADS * HEAD),
    "wv": (D, KV_HEADS * HEAD),
    "wo": (HEADS * HEAD, D),
    "w_gate": (D, FF),
    "w_up": (D, FF),
    "w_down": (FF, D),
}


def bump(key, n, height):
    away = (jnp.arange(n, dtype=jnp.int32) - jax.random.randint(key, (), 0, n, jnp.int32)) % n
    return jnp.where(away < n // 8, height, 1.0)


def together(key, own, strength):
    shared = jax.random.normal(key, own.shape[1:], jnp.float32)
    return (own + strength * shared) * lax.rsqrt(1 + strength * strength)


def setup_inputs(seed: int = 0, part: int = 0) -> dict:
    kx, kdy, ka, kb, kz, kf, kh, kl, *kw = jax.random.split(jax.random.key(seed), 8 + len(NAMES))
    kx, kdy, ka, kb = (jax.random.fold_in(k, part) for k in (kx, kdy, ka, kb))
    shape = (SEQUENCES, TOKENS, D)
    much_x, much_dy = jax.random.uniform(kz, (2,), jnp.float32, 0.0, 1.0)
    loud = 2.0 ** jax.random.uniform(jax.random.fold_in(kz, 1), (), jnp.float32, -1.0, 2.0)
    halves = 2.0 ** jax.random.uniform(kl, (2,), jnp.float32, -1.0, 1.0)
    times = {"wq": 1.0, "wk": 1.0, "wv": 2.0, "wo": halves[0], "w_gate": 1.0, "w_up": bump(kh, FF, 4.0), "w_down": halves[1]}
    x = together(ka, jax.random.normal(kx, shape, jnp.float32), much_x) * bump(kf, D, 4.0)
    dy = together(kb, jax.random.normal(kdy, shape, jnp.float32), much_dy)
    drawn = {"x": x.astype(jnp.bfloat16), "dy": (loud * dy * (SEQUENCES * TOKENS) ** -0.5).astype(jnp.bfloat16)}
    for key, name in zip(kw, NAMES, strict=True):
        drawn[name] = (jax.random.normal(key, SHAPES[name], jnp.float32) * SHAPES[name][0] ** -0.5 * times[name]).astype(jnp.bfloat16)
    return drawn


def matmul(a, w):
    return jnp.dot(a, w, preferred_element_type=jnp.float32).astype(jnp.bfloat16)


def normed(h):
    wide = h.astype(jnp.float32)
    scale = lax.rsqrt(jnp.mean(wide**2, -1, keepdims=True) + 1e-6)
    return (wide * scale).astype(jnp.bfloat16)


def turned(t, theta):
    half = t.shape[-1] // 2
    angle = jnp.arange(t.shape[0], dtype=jnp.float32)[:, None] * theta ** (-jnp.arange(half, dtype=jnp.float32) / half)
    cos, sin = jnp.cos(angle)[:, None], jnp.sin(angle)[:, None]
    a, b = t[..., :half].astype(jnp.float32), t[..., half:].astype(jnp.float32)
    return jnp.concatenate([a * cos - b * sin, b * cos + a * sin], -1).astype(jnp.bfloat16)


def seen_by(q, k, v):
    tokens, kv = q.shape[0], k.shape[1]
    q = q.reshape(tokens, kv, -1, q.shape[-1])
    scores = jnp.einsum("tgsd,ugd->gstu", q.astype(jnp.float32), k.astype(jnp.float32)) * q.shape[-1] ** -0.5
    place = jnp.arange(tokens)
    weights = jax.nn.softmax(jnp.where(place[:, None] >= place, scores, -jnp.inf), -1).astype(jnp.bfloat16)
    return jnp.einsum("gstu,ugd->tgsd", weights.astype(jnp.float32), v.astype(jnp.float32)).astype(jnp.bfloat16).reshape(tokens, -1)


def layer(h, w):
    a = normed(h)
    q, k = (turned(matmul(a, w[name]).reshape(h.shape[0], -1, HEAD), THETA) for name in ("wq", "wk"))
    h = h + matmul(seen_by(q, k, matmul(a, w["wv"]).reshape(h.shape[0], -1, HEAD)), w["wo"])
    b = normed(h)
    gate = jnp.dot(b, w["w_gate"], preferred_element_type=jnp.float32)
    up = jnp.dot(b, w["w_up"], preferred_element_type=jnp.float32)
    return h + matmul((jax.nn.silu(gate) * up).astype(jnp.bfloat16), w["w_down"])


def reference(x, dy, wq, wk, wv, wo, w_gate, w_up, w_down):
    weights = dict(zip(NAMES, (wq, wk, wv, wo, w_gate, w_up, w_down), strict=True))

    def take(so_far, sequence):
        h, by_y = sequence
        _, back = jax.vjp(lambda w, h: layer(h, w), weights, h)
        by_weights, by_h = back(by_y)
        return jax.tree.map(lambda total, term: total + term.astype(jnp.float32), so_far, by_weights), by_h

    none_yet = {name: jnp.zeros(w.shape, jnp.float32) for name, w in weights.items()}
    by_weights, by_x = lax.scan(take, none_yet, (x, dy))
    return (by_x, *(by_weights[name].astype(jnp.bfloat16) for name in NAMES))
```

```python
import functools

import jax
import jax.numpy as jnp
import numpy as np
from jax import lax
from jax.experimental import pallas as pl
from jax.experimental.pallas import tpu as pltpu
from jax.sharding import PartitionSpec as P

NEG = -1e30
HIDDEN = 2 * NEG
LOG2E = 1.4426950408889634
MIB = 2**20
VMEM = 56 * MIB
STRIP = 512
KEYS = 512
QUERIES, QUERIES_BACK = 1024, 512
HEAD = 128
SUM_ROWS = 8
SCALE = HEAD**-0.5
E = SCALE * LOG2E


def _dot(a, b, ca, cb):
    return lax.dot_general(a, b, (((ca,), (cb,)), ((), ())), preferred_element_type=jnp.float32)


_nn, _nt, _tn = (functools.partial(_dot, ca=ca, cb=cb) for ca, cb in ((1, 0), (1, 1), (0, 0)))


def work(gflops, megabytes):
    return pl.CostEstimate(flops=gflops * 10**9, bytes_accessed=megabytes * 10**6, transcendentals=0)


def _seen(iq, bq):
    first = iq * bq
    return lax.div(first + 1, KEYS), lax.div(first + bq - 1 + KEYS, KEYS)


def _gap(cols, bq):
    return lax.rem(lax.broadcasted_iota(jnp.int32, (KEYS, cols), 1), bq) - lax.broadcasted_iota(jnp.int32, (KEYS, cols), 0)


def _row(ref):
    return jnp.concatenate([ref[n : n + 1, :] for n in range(ref.shape[0])], axis=1)


def _forward(q_ref, k_ref, v_ref, o_ref, lse_ref, top_s, mix_s, gap_s):
    g, bq, d = q_ref.shape
    cols = g * bq
    iq = pl.program_id(0)
    strips = range(0, cols, STRIP)
    gap_s[...] = _gap(cols, bq)
    top_s[...] = jnp.full_like(top_s, NEG)
    mix_s[...] = jnp.zeros_like(mix_s)
    ones = jnp.ones((SUM_ROWS, KEYS), k_ref.dtype)

    def block(j, masked):
        here = pl.ds(j * KEYS, KEYS)
        scores = [_nt(k_ref[here, :], q_ref[...].reshape(cols, d)[at : at + STRIP, :]) for at in strips]
        weights, keeps = [], []
        for at, s in zip(strips, scores):
            if masked:
                s = jnp.where(gap_s[:, at : at + STRIP] >= j * KEYS - iq * bq, s, HIDDEN)
            old = top_s[:, at : at + STRIP]
            top = jnp.maximum(old, s.max(axis=0, keepdims=True))
            top_s[:, at : at + STRIP] = top
            weights.append(jnp.exp2((s - top) * E).astype(k_ref.dtype))
            keeps.append(jnp.exp2((old - top) * E))
        for at, p, keep in zip(strips, weights, keeps):
            values = jnp.concatenate([v_ref[here, :].T, ones], axis=0)
            mix_s[:, at : at + STRIP] = mix_s[:, at : at + STRIP] * keep + _nn(values, p)

    whole, last = _seen(iq, bq)
    loop(0, whole, lambda j: block(j, False))
    loop(whole, last, lambda j: block(j, True))
    total = mix_s[d : d + 1, :]
    o_ref[...] = (mix_s[:d, :] * (1 / total)).T.reshape(g, bq, d).astype(o_ref.dtype)
    lse = top_s[...] * SCALE + jnp.log(total)
    for n in range(g):
        lse_ref[n : n + 1, :] = lse[:, n * bq : (n + 1) * bq]


def _cost(q, width):
    g, s, d = q.shape
    return pl.CostEstimate(flops=2 * g * s * s * width, transcendentals=g * s * s, bytes_accessed=4 * q.size * q.dtype.itemsize)


def attend(q, k, v):
    g, s, d = q.shape
    bq = QUERIES
    queries = pl.BlockSpec((g, bq, d), lambda i: (0, i, 0))
    keys = pl.BlockSpec((s, d), lambda i: (0, 0))
    return pl.pallas_call(
        _forward, grid=(s // bq,), in_specs=[queries, keys, keys], out_specs=[queries, pl.BlockSpec((g, bq), lambda i: (0, i))],
        scratch_shapes=[pltpu.VMEM((1, g * bq), jnp.float32), pltpu.VMEM((d + SUM_ROWS, g * bq), jnp.float32), pltpu.VMEM((KEYS, g * bq), jnp.int32)],
        out_shape=[jax.ShapeDtypeStruct(q.shape, q.dtype), jax.ShapeDtypeStruct((g, s), jnp.float32)],
        compiler_params=pltpu.CompilerParams(dimension_semantics=("arbitrary",), vmem_limit_bytes=VMEM), cost_estimate=_cost(q, 2 * d), name="attend",
    )(q, k, v)


def _backward(q_ref, k_ref, v_ref, do_ref, lse_ref, delta_ref, cos_ref, sin_ref, dq_ref, dk_ref, dv_ref, dq_s, dk_s, dv_s, gap_s):
    g, bq, d = q_ref.shape
    cols, low = g * bq, q_ref.dtype
    iq = pl.program_id(0)
    strips = range(0, cols, STRIP)

    @pl.when(iq == 0)
    def _():
        gap_s[...] = _gap(cols, bq)
        dk_s[...] = jnp.zeros_like(dk_s)
        dv_s[...] = jnp.zeros_like(dv_s)

    dq_s[...] = jnp.zeros_like(dq_s)
    lses, deltas = _row(lse_ref) * LOG2E, _row(delta_ref)

    def block(j, masked):
        here = pl.ds(j * KEYS, KEYS)
        qs = [q_ref[...].reshape(cols, d)[at : at + STRIP, :] for at in strips]
        dos = [do_ref[...].reshape(cols, d)[at : at + STRIP, :] for at in strips]
        scores = [_nt(k_ref[here, :], x) for x in qs]
        dps = [_nt(v_ref[here, :], x) for x in dos]
        for n, at in enumerate(strips):
            p = jnp.exp2(scores[n] * E - lses[:, at : at + STRIP])
            if masked:
                p = jnp.where(gap_s[:, at : at + STRIP] >= j * KEYS - iq * bq, p, 0.0)
            ds = (p * (dps[n] - deltas[:, at : at + STRIP])).astype(low)
            dv_s[here, :] += _nn(p.astype(low), dos[n])
            dk_s[here, :] += _nn(ds, qs[n])
            dq_s[:, at : at + STRIP] += _nn(k_ref[here, :].T, ds)

    whole, last = _seen(iq, bq)
    loop(0, whole, lambda j: block(j, False))
    loop(whole, last, lambda j: block(j, True))
    here = pl.ds(iq * bq, bq)
    by_q = (dq_s[...] * SCALE).T
    cos, sin = cos_ref[here, :], sin_ref[here, :]
    for n in range(g):
        dq_ref[n] = turn(by_q[n * bq : (n + 1) * bq, :], cos, -sin)

    @pl.when(iq == pl.num_programs(0) - 1)
    def _():
        dk_ref[...] = turn(dk_s[...] * SCALE, cos_ref[...], -sin_ref[...])
        dv_ref[...] = dv_s[...].astype(dv_ref.dtype)


def attend_bwd(q, k, v, d_out, lse, delta, cos, sin):
    g, s, d = q.shape
    bq = QUERIES_BACK
    queries = pl.BlockSpec((g, bq, d), lambda i: (0, i, 0))
    keys = pl.BlockSpec((s, d), lambda i: (0, 0))
    table = pl.BlockSpec(cos.shape, lambda i: (0, 0))
    stats = pl.BlockSpec((g, bq), lambda i: (0, i))
    return pl.pallas_call(
        _backward, grid=(s // bq,), in_specs=[queries, keys, keys, queries, stats, stats, table, table], out_specs=[queries, keys, keys],
        scratch_shapes=[pltpu.VMEM((d, g * bq), jnp.float32), pltpu.VMEM((s, d), jnp.float32), pltpu.VMEM((s, d), jnp.float32),
                        pltpu.VMEM((KEYS, g * bq), jnp.int32)],
        out_shape=[jax.ShapeDtypeStruct(t.shape, t.dtype) for t in (q, k, v)],
        compiler_params=pltpu.CompilerParams(dimension_semantics=("arbitrary",), vmem_limit_bytes=VMEM), cost_estimate=_cost(q, 5 * d), name="attend_bwd",
    )(q, k, v, d_out, lse, delta, cos, sin)


THETA = 10000
NAMES = ("wq", "wk", "wv", "wo", "w_gate", "w_up", "w_down")
EPS = 1e-6
LOW = jnp.bfloat16
BLOCK = 256
SLICE = 512
HBM = pl.BlockSpec(memory_space=pltpu.HBM)


def normed(h):
    wide = h.astype(jnp.float32)
    scale = lax.rsqrt(jnp.mean(wide**2, -1, keepdims=True) + EPS)
    return (wide * scale).astype(jnp.bfloat16)


def place():
    me = lax.axis_index("tp")
    x, y, c = lax.div(me, 4), lax.rem(lax.div(me, 2), 2), lax.rem(me, 2)
    return me, (x, y, c), (me + 4 * (1 - 2 * x), me + 2 * (1 - 2 * y), me + 1 - 2 * c)


def greet(neighbours):
    barrier = pltpu.get_barrier_semaphore()
    for device in neighbours:
        pl.semaphore_signal(barrier, inc=1, device_id={"tp": device}, device_id_type=pl.DeviceIdType.MESH)
    pl.semaphore_wait(barrier, len(neighbours))


def send(src, dst, sems, n, device):
    return pltpu.make_async_remote_copy(src_ref=src, dst_ref=dst, send_sem=sems[0].at[n], recv_sem=sems[1].at[n], device_id={"tp": device},
                                        device_id_type=pl.DeviceIdType.MESH)


def rows_of(device, half=None):
    if half is None:
        return pl.ds(pl.multiple_of(device * BLOCK, BLOCK), BLOCK)
    return pl.ds(pl.multiple_of(device * BLOCK + half * (BLOCK // 2), BLOCK // 2), BLOCK // 2)


def loop(start, end, f):
    def step(i, _):
        f(i)

    lax.fori_loop(start, end, step, None)


HALF = BLOCK // 2
CHIP = 2 * BLOCK
GROUPS = 4


class Gather:
    def __init__(self, own_ref, all_ref, store, local, kept, sems):
        self.own_ref, self.all_ref, self.store, self.local, self.kept, self.sems = own_ref, all_ref, store, local, kept, sems
        _, (x, y, c), (dx, dy, dc) = place()
        self.at, self.near = (x, y, c), (dx, dy, dc)
        slot = lambda group, i, n=1: store.at[pl.ds(pl.multiple_of(group * CHIP + i * HALF, HALF), n * HALF)]
        self.own = slot(0, 2 * c, 2)
        mine = (slot(0, 2 * c), slot(0, 2 * c + 1))
        x1, x2, y1, y2, d0, d1 = (slot(g, i) for g, i in ((1, c), (2, c), (1, 2 + c), (2, 2 + c), (3, 2 * c), (3, 2 * c + 1)))
        steps = [(self.own, self.own, dc), (mine[1], x1, dx), (mine[0], x2, dx), (mine[0], y1, dy), (mine[1], y2, dy), (y1, d0, dx), (x1, d1, dy),
                 *((t, t, dc) for t in (x1, y1, x2, y2, d0, d1))]
        self.copies = [send(a, b, sems, n, to) for n, (a, b, to) in enumerate(steps)]

    def begin(self, change=None):
        load = pltpu.make_async_copy(self.own_ref, self.own, self.local.at[0])
        load.start()
        load.wait()
        if change is not None:
            rows = 32

            def some(n):
                here = pl.ds(pl.multiple_of(2 * HALF * self.at[2] + n * rows, rows), rows)
                self.store[here, :] = change(self.store[here, :])

            loop(0, BLOCK // rows, some)
        greet(self.near)
        for n in (1, 3, 2, 4, 0):
            self.copies[n].start()

    def arrive(self, group):
        ways = [((), (0,)), ((3, 5, 8), (1, 6, 7), (7,), (8,)), ((2, 9), (4, 10), (9,), (10,)), ((5, 11), (6, 12), (11,), (12,))]
        for k, way in enumerate(ways):

            @pl.when(group == k)
            def _(way=way):
                for n, *onward in filter(len, way):
                    self.copies[n].wait_recv()
                    for m in onward:
                        self.copies[m].start()

        for i in range(GROUPS):
            self.keep(group, i).start()

    def rows(self, group, i):
        x, y, c = self.at
        mixed = (group == 1) | (group == 2)
        turn_x = jnp.where(mixed, 1 if i < 2 else 0, lax.div(group, 3))
        turn_y = jnp.where(mixed, 0 if i < 2 else 1, lax.div(group, 3))
        core = jnp.where(mixed, i % 2, i // 2)
        half = jnp.where(mixed, 2 - group if i < 2 else group - 1, i % 2)
        device = (x + turn_x * (1 - 2 * x)) * 4 + (y + turn_y * (1 - 2 * y)) * 2 + core
        return device * 2 + half

    def keep(self, group, i):
        here = pl.ds(pl.multiple_of(group * CHIP + i * HALF, HALF), HALF)
        there = pl.ds(pl.multiple_of(self.rows(group, i) * HALF, HALF), HALF)
        return pltpu.make_async_copy(self.store.at[here], self.all_ref.at[there], self.kept.at[group, i])

    def states(self, group):
        return self.store[pl.ds(pl.multiple_of(group * CHIP, CHIP), CHIP), :]

    def end(self):
        def some(group):
            for i in range(GROUPS):
                self.keep(group, i).wait()

        loop(0, GROUPS, some)
        for copy in self.copies:
            copy.wait_send()


def gather_scratch(tokens, d):
    dma = pltpu.SemaphoreType.DMA
    return [pltpu.VMEM((tokens, d), LOW), dma((1,)), dma((GROUPS, GROUPS)), dma((13,)), dma((13,))]


def turn(t, cos, sin):
    half = HEAD // 2
    other = jnp.concatenate([t[:, half:], t[:, :half]], axis=1)
    return (t * jnp.concatenate([cos, cos], axis=1) + other * jnp.concatenate([-sin, sin], axis=1)).astype(LOW)


def angles(tokens):
    half = HEAD // 2
    angle = np.arange(tokens, dtype=np.float32)[:, None] * THETA ** (-np.arange(half, dtype=np.float32) / half)
    return jnp.asarray(np.cos(angle), jnp.float32), jnp.asarray(np.sin(angle), jnp.float32)


def _project(own_ref, wq_ref, wk_ref, wv_ref, cos_ref, sin_ref, all_ref, q_ref, k_ref, v_ref, store, local, kept, ssem, rsem, wq, wk, wv, wsem):
    gather = Gather(own_ref, all_ref, store, local, kept, (ssem, rsem))
    loads = [pltpu.make_async_copy(a, b, wsem.at[n]) for n, (a, b) in enumerate(((wq_ref, wq), (wk_ref, wk), (wv_ref, wv)))]
    for load in loads:
        load.start()
    gather.begin(normed)
    for load in loads:
        load.wait()

    def group(k):
        gather.arrive(k)

        def body(*refs):
            coses, sins, qs, ks, vs = (refs[n * GROUPS : (n + 1) * GROUPS] for n in range(5))
            t = gather.states(k)
            by_q, by_k, by_v = (_nn(t, w[...]).astype(LOW).astype(jnp.float32) for w in (wq, wk, wv))
            for i in range(GROUPS):
                rows = slice(i * HALF, (i + 1) * HALF)
                cos, sin = coses[i][...], sins[i][...]
                for n in range(q_ref.shape[0]):
                    qs[i][n] = turn(by_q[rows, n * HEAD : (n + 1) * HEAD], cos, sin)
                ks[i][...] = turn(by_k[rows], cos, sin)
                vs[i][...] = by_v[rows].astype(LOW)

        heads, one, table = [], [], []
        for i in range(GROUPS):
            at = gather.rows(k, i)
            heads.append(pl.BlockSpec((q_ref.shape[0], HALF, HEAD), lambda j, at=at: (0, at, 0)))
            one.append(pl.BlockSpec((HALF, HEAD), lambda j, at=at: (at, 0)))
            table.append(pl.BlockSpec((HALF, cos_ref.shape[1]), lambda j, at=at: (at, 0)))
        pltpu.emit_pipeline(body, grid=(1,), in_specs=[*table, *table], out_specs=[*heads, *one, *one])(
            *(ref for ref in (cos_ref, sin_ref, q_ref, k_ref, v_ref) for _ in range(GROUPS)))

    loop(0, GROUPS, group)
    gather.end()


def project(own, wq, wk, wv, cos, sin):
    d, tokens = own.shape[1], cos.shape[0]
    one = jax.ShapeDtypeStruct((tokens, HEAD), LOW)
    return pl.pallas_call(
        _project, in_specs=[HBM] * 6, out_specs=[HBM] * 4,
        out_shape=[jax.ShapeDtypeStruct((tokens, d), LOW), jax.ShapeDtypeStruct((wq.shape[1] // HEAD, tokens, HEAD), LOW), one, one],
        scratch_shapes=[*gather_scratch(tokens, d), *(pltpu.VMEM(w.shape, LOW) for w in (wq, wk, wv)), pltpu.SemaphoreType.DMA((3,))],
        compiler_params=pltpu.CompilerParams(collective_id=0, has_side_effects=True, vmem_limit_bytes=VMEM),
        cost_estimate=work(70, 60), name="project",
    )(own, wq, wk, wv, cos, sin)


NARROW = 256


def _hidden(own_ref, by_hidden_ref, wg_ref, wu_ref, all_ref, hidden_ref, by_gate_ref, by_up_ref, store, local, kept, ssem, rsem, wg, wu, wsem):
    gather = Gather(own_ref, all_ref, store, local, kept, (ssem, rsem))
    tiles = wg.shape[0]

    def weights(n):
        cut = pl.ds(pl.multiple_of(n * NARROW, NARROW), NARROW)
        return [pltpu.make_async_copy(a.at[:, cut], b.at[n], wsem.at[i, n]) for i, (a, b) in enumerate(((wg_ref, wg), (wu_ref, wu)))]

    gather.begin()
    loop(0, tiles, lambda n: [copy.start() for copy in weights(n)] and None)

    def group(k):
        gather.arrive(k)

        def body(*refs):
            bys, hiddens, by_gates, by_ups = (refs[n * GROUPS : (n + 1) * GROUPS] for n in range(4))
            j = pl.program_id(0)

            @pl.when(k == 0)
            def _():
                for copy in weights(j):
                    copy.wait()

            t = gather.states(k)
            gate, up = _nn(t, wg[j]), _nn(t, wu[j])
            for i in range(GROUPS):
                rows = slice(i * HALF, (i + 1) * HALF)
                g, u, by = gate[rows], up[rows], bys[i][...].astype(jnp.float32)
                s = jax.nn.sigmoid(g)
                silu = g * s
                hiddens[i][...] = (silu * u).astype(LOW)
                by_ups[i][...] = (by * silu).astype(LOW)
                by_gates[i][...] = (by * u * (s + silu * (1 - s))).astype(LOW)

        piece = [pl.BlockSpec((HALF, NARROW), lambda j, at=gather.rows(k, i): (at, j)) for i in range(GROUPS)]
        pltpu.emit_pipeline(body, grid=(tiles,), in_specs=piece, out_specs=piece * 3)(
            *(ref for ref in (by_hidden_ref, hidden_ref, by_gate_ref, by_up_ref) for _ in range(GROUPS)))

    loop(0, GROUPS, group)
    gather.end()


def hidden_units(own, by_hidden, w_gate, w_up):
    tokens, units = by_hidden.shape
    d = own.shape[1]
    part = jax.ShapeDtypeStruct((tokens, units), LOW)
    kept = pltpu.VMEM((units // NARROW, d, NARROW), LOW)
    return pl.pallas_call(
        _hidden, in_specs=[HBM] * 4, out_specs=[HBM] * 4, out_shape=[jax.ShapeDtypeStruct((tokens, d), LOW), part, part, part],
        scratch_shapes=[*gather_scratch(tokens, d), kept, kept, pltpu.SemaphoreType.DMA((2, units // NARROW))],
        compiler_params=pltpu.CompilerParams(collective_id=1, has_side_effects=True, vmem_limit_bytes=63 * MIB),
        cost_estimate=work(90, 200), name="hidden_units",
    )(own, by_hidden, w_gate, w_up)


ACROSS, ALONG_X, ALONG_Y, OWN = range(4)
UNITS = 16


def _unit(u):
    pair = lax.div(u, 2)
    middle = (pair >= 2) & (pair < 6)
    chip = jnp.where(middle, 1 + lax.rem(pair, 2), jnp.where(pair < 2, ACROSS, OWN))
    late = jnp.where(pair >= 4, 1, 0)
    half = jnp.where(middle, lax.rem(lax.rem(pair, 2) + late, 2), lax.rem(pair, 2))
    return chip, 2 * half + lax.rem(u, 2)


def _reduce(take, fillers, finish, counts, *refs):
    groups = []
    for count in counts:
        groups.append(refs[:count])
        refs = refs[count:]
    a_refs, w_refs, extra_refs, fill_refs, out_refs, fill_outs, a_bufs, w_bufs = groups
    mine, theirs, far, along, passed, asem, wsem, esem, osem, ssem, rsem = refs
    slices = mine.shape[0]
    half = slices // 2
    me, (x, y, c), (dx, dy, dc) = place()
    nt = [w.shape[1] == SLICE and w_ref.shape[0] == slices * SLICE for w, w_ref in zip(w_bufs, w_refs)]
    cut = lambda n: pl.ds(pl.multiple_of(n * SLICE, SLICE), SLICE)

    def weight(i, n):
        return pltpu.make_async_copy(w_refs[i].at[cut(n)] if nt[i] else w_refs[i].at[:, cut(n)], w_bufs[i].at[n], wsem.at[i, n])

    chips = (dx + 2 * (1 - 2 * y), dx, dy, me)

    def load(m):
        copies = []
        for s, device in enumerate((chips[m], chips[m] + 1 - 2 * c)):
            for i, (ref, buf) in enumerate(zip(a_refs, a_bufs)):
                at = pl.ds(s * BLOCK, BLOCK)
                copies.append(pltpu.make_async_copy(ref.at[:, rows_of(device)], buf.at[m % 2, :, at], asem.at[m % 2, i, s]) if len(ref.shape) == 3 else
                              pltpu.make_async_copy(ref.at[rows_of(device)], buf.at[m % 2, at], asem.at[m % 2, i, s]))
        return copies

    def begin(copies):
        for copy in copies:
            copy.start()

    def finished(copies):
        for copy in copies:
            copy.wait()

    halves = (pl.ds(0, half), pl.ds(half, half))
    sems = (ssem, rsem)
    to_core = [[send(mine.at[h], theirs.at[m, h], sems, 2 * m + n, dc) for n, h in enumerate(halves)] for m in range(4)]
    to_far = [send(passed.at[ACROSS, h], far.at[h], sems, 8 + n, (dx, dy)[n]) for n, h in enumerate(halves)]
    to_x = [send(passed.at[ALONG_X, h], along.at[0, h], sems, 10 + n, dx) for n, h in enumerate(halves)]
    to_y = [send(passed.at[ALONG_Y, h], along.at[1, h], sems, 12 + n, dy) for n, h in enumerate(halves)]

    begin(load(ACROSS))
    loop(0, slices, lambda n: begin([weight(i, n) for i in range(len(w_refs))]))
    begin(load(ALONG_X))
    greet((dx, dy, dc))

    def join(m, h, copy, by_far=False):
        to_core[m][h].wait_recv()
        if by_far:
            to_far[h].wait_recv()

        def one(i):
            n = h * half + i
            t = passed[m, n].astype(jnp.float32) + theirs[m, n].astype(jnp.float32)
            if by_far:
                t += far[n].astype(jnp.float32)
            passed[m, n] = t.astype(LOW)

        loop(0, half, one)
        copy.start()

    first = {0: lambda: finished(load(ACROSS)), 4: lambda: (to_core[ACROSS][0].wait_send(), finished(load(ALONG_X)), begin(load(ALONG_Y))),
             6: lambda: (to_core[ACROSS][1].wait_send(), finished(load(ALONG_Y))), 8: lambda: to_core[ALONG_Y][1].wait_send(),
             10: lambda: (to_core[ALONG_X][0].wait_send(), begin(load(OWN)), fillers and fillers[0](fill_refs, fill_outs) and None),
             12: lambda: (to_core[ALONG_Y][0].wait_send(), finished(load(OWN))), 14: lambda: to_core[ALONG_X][1].wait_send()}
    then = {1: lambda: to_core[ACROSS][0].start(), 2: lambda: join(ACROSS, 0, to_far[0]), 3: lambda: to_core[ACROSS][1].start(),
            4: lambda: join(ACROSS, 1, to_far[1]), 5: lambda: to_core[ALONG_X][0].start(), 6: lambda: join(ALONG_X, 0, to_x[0]),
            7: lambda: to_core[ALONG_Y][1].start(), 8: lambda: join(ALONG_Y, 1, to_y[1]), 9: lambda: to_core[ALONG_X][1].start(),
            10: lambda: join(ALONG_X, 1, to_x[1], True), 11: lambda: to_core[ALONG_Y][0].start(), 12: lambda: join(ALONG_Y, 0, to_y[0], True),
            13: lambda: to_core[OWN][0].start(), 15: lambda: to_core[OWN][1].start()}

    def unit(u):
        m, quarter = _unit(u)
        slot = lax.rem(m, 2)
        for at, act in first.items():
            pl.when(u == at)(lambda act=act: act() and None)

        def one(i):
            n = quarter * (half // 2) + i

            @pl.when(u < 4)
            def _():
                finished([weight(i, n) for i in range(len(w_refs))])

            acc = sum(_dot(t, w[n], 1, 1 if t_ else 0) for t, w, t_ in zip(take([b.at[slot] for b in a_bufs]), w_bufs, nt)).astype(LOW)
            passed[m, n] = acc[:BLOCK]
            mine[n] = acc[BLOCK:]

        loop(0, half // 2, one)
        for at, act in then.items():
            pl.when(u == at)(lambda act=act: act() and None)

    loop(0, UNITS, unit)
    for fill in fillers[1:]:
        fill(fill_refs, fill_outs)

    for copy in (*to_core[OWN], *to_far):
        copy.wait_send()
    extras = [passed.at[ACROSS], mine][: len(extra_refs)]
    slice_copies = lambda pairs, sem, n: [pltpu.make_async_copy(r.at[:, cut(n)], b.at[n], sem.at[i, n]) for i, (r, b) in enumerate(pairs)]
    loads = list(zip(extra_refs, extras))
    loop(0, slices, lambda n: begin(slice_copies(loads, esem, n)))
    loop(0, slices, lambda n: finished(slice_copies(loads, esem, n)))
    for copy in (*to_x, *to_y):
        copy.wait_send()
    for copy in (*to_core[OWN], *to_x, *to_y):
        copy.wait_recv()

    def sum_of(n):
        return sum(t.astype(jnp.float32) for t in (passed[OWN, n], theirs[OWN, n], along[0, n], along[1, n]))

    results = finish(slices, sum_of, extras, theirs.at[ACROSS])

    def put(n):
        return [pltpu.make_async_copy(b.at[n], r.at[:, cut(n)], osem.at[i, n]) for i, (r, b) in enumerate(zip(out_refs, results))]

    loop(0, slices, lambda n: begin(put(n)))
    loop(0, slices, lambda n: finished(put(n)))


def reduce(name, number, take, terms, weights, extras, outs, finish, gflops, fillers=(), fill=(), fill_outs=()):
    d = extras[0].shape[1]
    slices = d // SLICE
    state = (slices, BLOCK, SLICE)
    both = 2 * BLOCK
    blocks = [(2, t.shape[0], both, t.shape[2]) if t.ndim == 3 else (2, both, t.shape[1]) for t in terms]
    kept = [(slices, SLICE, w.shape[1]) if w.shape[0] == d else (slices, w.shape[0], SLICE) for w in weights]
    dma = pltpu.SemaphoreType.DMA
    counts = (len(terms), len(weights), len(extras), len(fill), outs, len(fill_outs), len(terms), len(weights))
    low = lambda *shape: pltpu.VMEM(shape, LOW)
    return pl.pallas_call(
        functools.partial(_reduce, take, fillers, finish, counts),
        in_specs=[HBM] * sum(counts[:4]), out_specs=[HBM] * (outs + len(fill_outs)),
        out_shape=[jax.ShapeDtypeStruct((BLOCK, d), LOW)] * outs + [jax.ShapeDtypeStruct(s, LOW) for s in fill_outs],
        scratch_shapes=[*(low(*s) for s in blocks), *(low(*s) for s in kept), low(*state), low(4, *state), low(*state), low(2, *state), low(4, *state),
                        dma((2, len(terms), 2)), dma((len(weights), slices)), dma((len(extras), slices)), dma((outs, slices)), dma((14,)), dma((14,))],
        compiler_params=pltpu.CompilerParams(collective_id=number, has_side_effects=True, vmem_limit_bytes=63 * MIB),
        cost_estimate=work(gflops, 60), name=name,
    )(*terms, *weights, *extras, *fill)


def finish_norm(slices, sum_of, extras, spare):
    (states,) = extras

    def one(n, squares):
        h = (states[n].astype(jnp.float32) + sum_of(n)).astype(LOW)
        states[n] = h
        wide = h.astype(jnp.float32)
        return squares + jnp.sum(wide * wide, -1, keepdims=True)

    squares = lax.fori_loop(0, slices, one, jnp.zeros((BLOCK, 1), jnp.float32))
    scale = lax.rsqrt(squares / (slices * SLICE) + EPS)

    def two(n):
        spare[n] = (states[n].astype(jnp.float32) * scale).astype(LOW)

    loop(0, slices, two)
    return states, spare


def finish_back(slices, sum_of, extras, spare):
    states, rest = extras

    def one(n, so_far):
        squares, across = so_far
        h, g = states[n].astype(jnp.float32), sum_of(n)
        return squares + jnp.sum(h * h, -1, keepdims=True), across + jnp.sum(h * g, -1, keepdims=True)

    zero = jnp.zeros((BLOCK, 1), jnp.float32)
    squares, across = lax.fori_loop(0, slices, one, (zero, zero))
    size = slices * SLICE
    scale = lax.rsqrt(squares / size + EPS)
    back = scale * scale * scale * (across / size)

    def two(n):
        by = sum_of(n) * scale - states[n].astype(jnp.float32) * back
        rest[n] = (rest[n].astype(jnp.float32) + by).astype(LOW)

    loop(0, slices, two)
    return (rest,)


def side_by_side(r):
    return jnp.concatenate([r[n] for n in range(r.shape[0])], axis=1)


def heads_side_by_side(refs):
    return [side_by_side(refs[0])]


def as_they_are(refs):
    return [r[...] for r in refs]


def heads_and_two(refs):
    q, k, v = refs
    return [side_by_side(q), k[...], v[...]]


WIDE = 512


def fill_by_hidden(part, refs, outs):
    dy_ref, wd_ref = refs
    (units, d), tokens = wd_ref.shape, dy_ref.shape[0]
    rows, wide = tokens // 2, units // 4

    def body(dy, w, out):
        out[...] = _nt(dy[...], w[...]).astype(LOW)

    pltpu.emit_pipeline(body, grid=(units // wide,), in_specs=[pl.BlockSpec((rows, d), lambda j: (part, 0)), pl.BlockSpec((wide, d), lambda j: (j, 0))],
                        out_specs=[pl.BlockSpec((rows, wide), lambda j: (part, j))])(dy_ref, wd_ref, outs[0])


def fill_by_wo(refs, outs):
    heads_ref, all_h_ref = refs[:2]
    g, tokens, _ = heads_ref.shape

    def body(heads, h, out):
        out[...] = _tn(side_by_side(heads), h[...]).astype(LOW)

    pltpu.emit_pipeline(body, grid=(all_h_ref.shape[1] // WIDE,), in_specs=[pl.BlockSpec((g, tokens, HEAD), lambda j: (0, 0, 0)),
                                                                          pl.BlockSpec((tokens, WIDE), lambda j: (0, j))],
                        out_specs=[pl.BlockSpec((g * HEAD, WIDE), lambda j: (0, j))])(heads_ref, all_h_ref, outs[0])


def fill_by_rest(refs, outs):
    a_ref, q_ref, k_ref, v_ref = refs[2:]
    g, tokens, _ = q_ref.shape
    one = pl.BlockSpec((tokens, HEAD), lambda j: (0, 0))
    narrow = pl.BlockSpec((WIDE, HEAD), lambda j: (j, 0))

    def body(a, q, k, v, by_q, by_k, by_v):
        t = _tn(a[...], jnp.concatenate([side_by_side(q), k[...], v[...]], axis=1)).astype(LOW)
        by_q[...], by_k[...], by_v[...] = t[:, : g * HEAD], t[:, g * HEAD : (g + 1) * HEAD], t[:, (g + 1) * HEAD :]

    pltpu.emit_pipeline(body, grid=(a_ref.shape[1] // WIDE,),
                        in_specs=[pl.BlockSpec((tokens, WIDE), lambda j: (0, j)), pl.BlockSpec((g, tokens, HEAD), lambda j: (0, 0, 0)), one, one],
                        out_specs=[pl.BlockSpec((WIDE, g * HEAD), lambda j: (j, 0)), narrow, narrow])(a_ref, q_ref, k_ref, v_ref, *outs[1:])


def _by_heads(h, wo, out):
    t = _nt(h[...], wo[...]).astype(LOW)
    for n in range(out.shape[0]):
        out[n] = t[:, n * HEAD : (n + 1) * HEAD]


def by_heads(all_h, wo):
    tokens, d = all_h.shape
    rows, g = 512, wo.shape[0] // HEAD
    return pl.pallas_call(
        _by_heads, grid=(tokens // rows,), in_specs=[pl.BlockSpec((rows, d), lambda i: (i, 0)), pl.BlockSpec(wo.shape, lambda i: (0, 0))],
        out_specs=pl.BlockSpec((g, rows, HEAD), lambda i: (0, i, 0)), out_shape=jax.ShapeDtypeStruct((g, tokens, HEAD), LOW),
        compiler_params=pltpu.CompilerParams(dimension_semantics=("arbitrary",), vmem_limit_bytes=VMEM),
        cost_estimate=pl.CostEstimate(flops=2 * tokens * d * wo.shape[0], bytes_accessed=2 * all_h.size, transcendentals=0), name="by_heads",
    )(all_h, wo)


def mm(eq, a, b):
    return jnp.einsum(eq, a, b, preferred_element_type=jnp.float32).astype(LOW)


def layer(x, dy, w):
    tokens, d = BLOCK * 8, x.shape[1]
    cos, sin = angles(tokens)
    a, q, k, v = project(x, w["wq"], w["wk"], w["wv"], cos, sin)
    dy_late, q = lax.optimization_barrier((dy, q))
    all_dy = lax.all_gather(dy_late, "tp", axis=0, tiled=True)
    heads, lse = attend(q, k, v)
    units = w["w_down"].shape[0]
    h, b_own, by_hidden = reduce("add_heads", 2, heads_side_by_side, [heads], [w["wo"]], [x], 2, finish_norm, 60,
                                 [functools.partial(fill_by_hidden, part) for part in range(2)], [all_dy, w["w_down"]], [(tokens, units)])
    b, hidden, by_gate, by_up = hidden_units(b_own, by_hidden, w["w_gate"], w["w_up"])
    (by_h,) = reduce("by_states", 3, as_they_are, [by_gate, by_up], [w["w_gate"], w["w_up"]], [h, dy], 1, finish_back, 80)
    all_h = lax.all_gather(by_h, "tp", axis=0, tiled=True)
    by_w = {"w_down": mm("tu,td->ud", hidden, all_dy), "w_gate": mm("td,tu->du", b, by_gate), "w_up": mm("td,tu->du", b, by_up)}
    by_out = by_heads(all_h, w["wo"])
    delta = (by_out.astype(jnp.float32) * heads.astype(jnp.float32)).sum(-1)
    by_q, by_k, by_v = attend_bwd(q, k, v, by_out, lse, delta, cos, sin)
    by_x, *rest = reduce("by_input", 4, heads_and_two, [by_q, by_k, by_v], [w["wq"], w["wk"], w["wv"]], [x, by_h], 1, finish_back, 60,
                         [fill_by_wo, fill_by_rest], [heads, all_h, a, by_q, by_k, by_v], [w[name].shape for name in ("wo", "wq", "wk", "wv")])
    by_w.update(zip(("wo", "wq", "wk", "wv"), rest))
    return by_x, by_w


def solution(mesh):
    def step(x, dy, *weights):
        by_x, by_w = layer(x[0], dy[0], dict(zip(NAMES, weights, strict=True)))
        return (by_x[None], *(by_w[name] for name in NAMES))

    states, by_columns, by_rows = P("dp", "tp", None), P(None, "tp"), P("tp", None)
    weights = (by_columns, by_columns, by_columns, by_rows, by_columns, by_columns, by_rows)
    own = tuple(P("dp", "tp") if spec == by_columns else P(("dp", "tp"), None) for spec in weights)
    return jax.shard_map(step, mesh=mesh, in_specs=(states, states, *weights), out_specs=(states, *own), check_vma=False)
```

```python
import functools

import jax
import jax.numpy as jnp
import numpy as np
from jax import lax
from jax.experimental import pallas as pl
from jax.experimental.pallas import tpu as pltpu
from jax.sharding import PartitionSpec as P

NEG = -1e30
HIDDEN = 2 * NEG
LOG2E = 1.4426950408889634
MIB = 2**20
VMEM, ALL_VMEM = 56 * MIB, 63 * MIB
STRIP = 512
KEYS = 512
QUERIES, QUERIES_BACK = 1024, 512
HEAD = 128
SUM_ROWS = 8
SCALE = HEAD**-0.5
E = SCALE * LOG2E


def _dot(a, b, ca, cb):
    return lax.dot_general(a, b, (((ca,), (cb,)), ((), ())), preferred_element_type=jnp.float32)


_nn, _nt, _tn = (functools.partial(_dot, ca=ca, cb=cb) for ca, cb in ((1, 0), (1, 1), (0, 0)))


def work(gflops, megabytes):
    return pl.CostEstimate(flops=gflops * 10**9, bytes_accessed=megabytes * 10**6, transcendentals=0)


def _seen(iq, bq):
    first = iq * bq
    return lax.div(first + 1, KEYS), lax.div(first + bq - 1 + KEYS, KEYS)


def _gap(cols, bq):
    return lax.rem(lax.broadcasted_iota(jnp.int32, (KEYS, cols), 1), bq) - lax.broadcasted_iota(jnp.int32, (KEYS, cols), 0)


def _row(ref):
    return jnp.concatenate([ref[n : n + 1, :] for n in range(ref.shape[0])], axis=1)


def _forward(q_ref, k_ref, v_ref, o_ref, lse_ref, top_s, mix_s, gap_s):
    g, bq, d = q_ref.shape
    cols = g * bq
    iq = pl.program_id(0)
    strips = range(0, cols, STRIP)
    gap_s[...] = _gap(cols, bq)
    top_s[...] = jnp.full_like(top_s, NEG)
    mix_s[...] = jnp.zeros_like(mix_s)
    ones = jnp.ones((SUM_ROWS, KEYS), k_ref.dtype)

    def block(j, masked):
        here = pl.ds(j * KEYS, KEYS)
        scores = [_nt(k_ref[here, :], q_ref[...].reshape(cols, d)[at : at + STRIP, :]) for at in strips]
        weights, keeps = [], []
        for at, s in zip(strips, scores):
            if masked:
                s = jnp.where(gap_s[:, at : at + STRIP] >= j * KEYS - iq * bq, s, HIDDEN)
            old = top_s[:, at : at + STRIP]
            top = jnp.maximum(old, s.max(axis=0, keepdims=True))
            top_s[:, at : at + STRIP] = top
            weights.append(jnp.exp2((s - top) * E).astype(k_ref.dtype))
            keeps.append(jnp.exp2((old - top) * E))
        for at, p, keep in zip(strips, weights, keeps):
            values = jnp.concatenate([v_ref[here, :].T, ones], axis=0)
            mix_s[:, at : at + STRIP] = mix_s[:, at : at + STRIP] * keep + _nn(values, p)

    whole, last = _seen(iq, bq)
    loop(0, whole, lambda j: block(j, False))
    loop(whole, last, lambda j: block(j, True))
    total = mix_s[d : d + 1, :]
    o_ref[...] = (mix_s[:d, :] * (1 / total)).T.reshape(g, bq, d).astype(o_ref.dtype)
    lse = top_s[...] * SCALE + jnp.log(total)
    for n in range(g):
        lse_ref[n : n + 1, :] = lse[:, n * bq : (n + 1) * bq]


def _cost(q, width):
    g, s, d = q.shape
    return pl.CostEstimate(flops=2 * g * s * s * width, transcendentals=g * s * s, bytes_accessed=4 * q.size * q.dtype.itemsize)


def _backward(q_ref, k_ref, v_ref, do_ref, lse_ref, delta_ref, cos_ref, sin_ref, dq_ref, dk_ref, dv_ref, dq_s, dk_s, dv_s, gap_s):
    g, bq, d = q_ref.shape
    cols, low = g * bq, q_ref.dtype
    iq = pl.program_id(0)
    strips = range(0, cols, STRIP)

    @pl.when(iq == 0)
    def _():
        gap_s[...] = _gap(cols, bq)
        dk_s[...] = jnp.zeros_like(dk_s)
        dv_s[...] = jnp.zeros_like(dv_s)

    dq_s[...] = jnp.zeros_like(dq_s)
    lses, deltas = _row(lse_ref) * LOG2E, _row(delta_ref)

    def block(j, masked):
        here = pl.ds(j * KEYS, KEYS)
        qs = [q_ref[...].reshape(cols, d)[at : at + STRIP, :] for at in strips]
        dos = [do_ref[...].reshape(cols, d)[at : at + STRIP, :] for at in strips]
        scores = [_nt(k_ref[here, :], x) for x in qs]
        dps = [_nt(v_ref[here, :], x) for x in dos]
        for n, at in enumerate(strips):
            p = jnp.exp2(scores[n] * E - lses[:, at : at + STRIP])
            if masked:
                p = jnp.where(gap_s[:, at : at + STRIP] >= j * KEYS - iq * bq, p, 0.0)
            ds = (p * (dps[n] - deltas[:, at : at + STRIP])).astype(low)
            dv_s[here, :] += _nn(p.astype(low), dos[n])
            dk_s[here, :] += _nn(ds, qs[n])
            dq_s[:, at : at + STRIP] += _nn(k_ref[here, :].T, ds)

    whole, last = _seen(iq, bq)
    loop(0, whole, lambda j: block(j, False))
    loop(whole, last, lambda j: block(j, True))
    here = pl.ds(iq * bq, bq)
    by_q = (dq_s[...] * SCALE).T
    cos, sin = cos_ref[here, :], sin_ref[here, :]
    for n in range(g):
        dq_ref[n] = turn(by_q[n * bq : (n + 1) * bq, :], cos, -sin)

    @pl.when(iq == pl.num_programs(0) - 1)
    def _():
        dk_ref[...] = turn(dk_s[...] * SCALE, cos_ref[...], -sin_ref[...])
        dv_ref[...] = dv_s[...].astype(dv_ref.dtype)


def attend_bwd(q, k, v, d_out, lse, delta, cos, sin):
    g, s, d = q.shape
    bq = QUERIES_BACK
    queries = pl.BlockSpec((g, bq, d), lambda i: (0, i, 0))
    keys = pl.BlockSpec((s, d), lambda i: (0, 0))
    table = pl.BlockSpec(cos.shape, lambda i: (0, 0))
    stats = pl.BlockSpec((g, bq), lambda i: (0, i))
    return pl.pallas_call(
        _backward, grid=(s // bq,), in_specs=[queries, keys, keys, queries, stats, stats, table, table], out_specs=[queries, keys, keys],
        scratch_shapes=[pltpu.VMEM((d, g * bq), jnp.float32), pltpu.VMEM((s, d), jnp.float32), pltpu.VMEM((s, d), jnp.float32),
                        pltpu.VMEM((KEYS, g * bq), jnp.int32)],
        out_shape=[jax.ShapeDtypeStruct(t.shape, t.dtype) for t in (q, k, v)],
        compiler_params=pltpu.CompilerParams(dimension_semantics=("arbitrary",), vmem_limit_bytes=VMEM), cost_estimate=_cost(q, 5 * d), name="attend_bwd",
    )(q, k, v, d_out, lse, delta, cos, sin)


THETA = 10000
NAMES = ("wq", "wk", "wv", "wo", "w_gate", "w_up", "w_down")
EPS = 1e-6
LOW = jnp.bfloat16
BLOCK = 256
SLICE = 512
HBM = pl.BlockSpec(memory_space=pltpu.HBM)


def normed(h):
    wide = h.astype(jnp.float32)
    scale = lax.rsqrt(jnp.mean(wide**2, -1, keepdims=True) + EPS)
    return (wide * scale).astype(jnp.bfloat16)


def place():
    me = lax.axis_index("tp")
    x, y, c = lax.div(me, 4), lax.rem(lax.div(me, 2), 2), lax.rem(me, 2)
    return me, (x, y, c), (me + 4 * (1 - 2 * x), me + 2 * (1 - 2 * y), me + 1 - 2 * c)


def greet(neighbours):
    barrier = pltpu.get_barrier_semaphore()
    for device in neighbours:
        pl.semaphore_signal(barrier, inc=1, device_id={"tp": device}, device_id_type=pl.DeviceIdType.MESH)
    pl.semaphore_wait(barrier, len(neighbours))


def send(src, dst, sems, n, device):
    return pltpu.make_async_remote_copy(src_ref=src, dst_ref=dst, send_sem=sems[0].at[n], recv_sem=sems[1].at[n], device_id={"tp": device},
                                        device_id_type=pl.DeviceIdType.MESH)


def rows_of(device, half=None):
    if half is None:
        return pl.ds(pl.multiple_of(device * BLOCK, BLOCK), BLOCK)
    return pl.ds(pl.multiple_of(device * BLOCK + half * (BLOCK // 2), BLOCK // 2), BLOCK // 2)


def loop(start, end, f):
    def step(i, _):
        f(i)

    lax.fori_loop(start, end, step, None)


HALF = BLOCK // 2
CHIP = 2 * BLOCK
GROUPS = 4


WAYS = [[(0,)], [(3, 5, 8), (1, 6, 7), (7,), (8,)], [(2, 9), (4, 10), (9,), (10,)], [(5, 11), (6, 12), (11,), (12,)]]


class Gather:
    def __init__(self, own_ref, all_ref, sems, local, store=None, kept=None):
        self.own_ref, self.all_ref, self.store, self.local, self.kept = own_ref, all_ref, store, local, kept
        me, (x, y, c), (dx, dy, dc) = place()
        self.at, self.near = (x, y, c), (dx, dy, dc)
        if store is None:
            half = lambda device, n: all_ref.at[pl.ds(pl.multiple_of(device * BLOCK + n * HALF, HALF), HALF)]
            self.own = own_ref
            mine = [own_ref.at[pl.ds(n * HALF, HALF)] for n in range(2)]
            x1, x2, y1, y2, d0, d1 = half(me, 1), half(me, 0), half(me, 0), half(me, 1), half(dy, 0), half(dx, 1)
            own, came = all_ref.at[rows_of(me)], [half(dx, 1), half(dy, 0), half(dx, 0), half(dy, 1)]
            came += [half(dx + 2 * (1 - 2 * y), n) for n in range(2)]
        else:
            slot = lambda group, i, n=1: store.at[pl.ds(pl.multiple_of(group * CHIP + i * HALF, HALF), n * HALF)]
            own = self.own = slot(0, 2 * c, 2)
            mine = (slot(0, 2 * c), slot(0, 2 * c + 1))
            came = x1, y1, x2, y2, d0, d1 = [slot(g, i) for g, i in ((1, c), (1, 2 + c), (2, c), (2, 2 + c), (3, 2 * c), (3, 2 * c + 1))]
        steps = [(self.own, own, dc), (mine[1], x1, dx), (mine[0], x2, dx), (mine[0], y1, dy), (mine[1], y2, dy), (came[1], d0, dx), (came[0], d1, dy),
                 *((t, t, dc) for t in came)]
        self.copies = [send(a, b, sems, n, to) for n, (a, b, to) in enumerate(steps)]

    def begin(self, change=None):
        load = pltpu.make_async_copy(self.own_ref, self.own, self.local.at[0])
        load.start()
        load.wait()
        if change is not None:
            rows = 32

            def some(n):
                here = pl.ds(pl.multiple_of(2 * HALF * self.at[2] + n * rows, rows), rows)
                self.store[here, :] = change(self.store[here, :])

            loop(0, BLOCK // rows, some)
        greet(self.near)
        self.start()

    def start(self):
        for n in (1, 3, 2, 4, 0):
            self.copies[n].start()

    def arrive(self, group):
        for k in range(GROUPS):
            pl.when(group == k)(functools.partial(self.take, k))
        for i in range(GROUPS):
            self.keep(group, i).start()

    def take(self, group):
        for n, *onward in WAYS[group]:
            self.copies[n].wait_recv()
            for m in onward:
                self.copies[m].start()

    def rows(self, group, i):
        x, y, c = self.at
        mixed = (group == 1) | (group == 2)
        turn_x = jnp.where(mixed, 1 if i < 2 else 0, lax.div(group, 3))
        turn_y = jnp.where(mixed, 0 if i < 2 else 1, lax.div(group, 3))
        core = jnp.where(mixed, i % 2, i // 2)
        half = jnp.where(mixed, 2 - group if i < 2 else group - 1, i % 2)
        device = (x + turn_x * (1 - 2 * x)) * 4 + (y + turn_y * (1 - 2 * y)) * 2 + core
        return device * 2 + half

    def keep(self, group, i):
        here = pl.ds(pl.multiple_of(group * CHIP + i * HALF, HALF), HALF)
        there = pl.ds(pl.multiple_of(self.rows(group, i) * HALF, HALF), HALF)
        return pltpu.make_async_copy(self.store.at[here], self.all_ref.at[there], self.kept.at[group, i])

    def states(self, group):
        return self.store[pl.ds(pl.multiple_of(group * CHIP, CHIP), CHIP), :]

    def end(self):
        def some(group):
            for i in range(GROUPS):
                self.keep(group, i).wait()

        if self.store is not None:
            loop(0, GROUPS, some)
        for copy in self.copies:
            copy.wait_send()


def gather_scratch(tokens, d):
    dma = pltpu.SemaphoreType.DMA
    return [pltpu.VMEM((tokens, d), LOW), dma((1,)), dma((GROUPS, GROUPS)), dma((13,)), dma((13,))]


def turn(t, cos, sin):
    half = HEAD // 2
    other = jnp.concatenate([t[:, half:], t[:, :half]], axis=1)
    return (t * jnp.concatenate([cos, cos], axis=1) + other * jnp.concatenate([-sin, sin], axis=1)).astype(LOW)


def angles(tokens):
    half = HEAD // 2
    angle = np.arange(tokens, dtype=np.float32)[:, None] * THETA ** (-np.arange(half, dtype=np.float32) / half)
    return jnp.asarray(np.cos(angle), jnp.float32), jnp.asarray(np.sin(angle), jnp.float32)


def _project(own_ref, dy_ref, wq_ref, wk_ref, wv_ref, cos_ref, sin_ref, all_ref, q_ref, k_ref, v_ref, all_dy_ref, o_ref, lse_ref, store, local, kept, ssem,
             rsem, wq, wk, wv, wsem, block, dy_ssem, dy_rsem, *scratch):
    gather = Gather(own_ref, all_ref, (ssem, rsem), local, store, kept)
    loads = [pltpu.make_async_copy(a, b, wsem.at[n]) for n, (a, b) in enumerate(((wq_ref, wq), (wk_ref, wk), (wv_ref, wv)))]
    for load in loads:
        load.start()
    gather.begin(normed)
    dy = Gather(dy_ref, all_dy_ref, (dy_ssem, dy_rsem), local)
    keep = pltpu.make_async_copy(dy_ref, block, local.at[0])
    keep.start()
    for load in loads:
        load.wait()
    keep.wait()
    keep = pltpu.make_async_copy(block, all_dy_ref.at[rows_of(lax.axis_index("tp"))], local.at[0])
    keep.start()

    def group(k):
        gather.arrive(k)
        pl.when(k == 1)(dy.start)

        def body(*refs):
            coses, sins, qs, ks, vs = (refs[n * GROUPS : (n + 1) * GROUPS] for n in range(5))
            t = gather.states(k)
            by_q, by_k, by_v = (_nn(t, w[...]).astype(LOW).astype(jnp.float32) for w in (wq, wk, wv))
            for i in range(GROUPS):
                rows = slice(i * HALF, (i + 1) * HALF)
                cos, sin = coses[i][...], sins[i][...]
                for n in range(q_ref.shape[0]):
                    qs[i][n] = turn(by_q[rows, n * HEAD : (n + 1) * HEAD], cos, sin)
                ks[i][...] = turn(by_k[rows], cos, sin)
                vs[i][...] = by_v[rows].astype(LOW)

        heads, one, table = [], [], []
        for i in range(GROUPS):
            at = gather.rows(k, i)
            heads.append(pl.BlockSpec((q_ref.shape[0], HALF, HEAD), lambda j, at=at: (0, at, 0)))
            one.append(pl.BlockSpec((HALF, HEAD), lambda j, at=at: (at, 0)))
            table.append(pl.BlockSpec((HALF, cos_ref.shape[1]), lambda j, at=at: (at, 0)))
        pltpu.emit_pipeline(body, grid=(1,), in_specs=[*table, *table], out_specs=[*heads, *one, *one])(
            *(ref for ref in (cos_ref, sin_ref, q_ref, k_ref, v_ref) for _ in range(GROUPS)))

    loop(0, GROUPS, group)
    g, tokens, d = q_ref.shape
    queries = pl.BlockSpec((g, QUERIES, d), lambda i: (0, i, 0))
    keys = pl.BlockSpec((tokens, d), lambda i: (0, 0))
    pltpu.emit_pipeline(lambda *refs: _forward(*refs, *scratch), grid=(tokens // QUERIES,), in_specs=[queries, keys, keys],
                        out_specs=[queries, pl.BlockSpec((g, QUERIES), lambda i: (0, i))])(q_ref, k_ref, v_ref, o_ref, lse_ref)
    for k in range(GROUPS):
        dy.take(k)
    keep.wait()
    dy.end()
    gather.end()


def project(own, dy, wq, wk, wv, cos, sin):
    d, tokens = own.shape[1], cos.shape[0]
    one, states = jax.ShapeDtypeStruct((tokens, HEAD), LOW), jax.ShapeDtypeStruct((tokens, d), LOW)
    g = wq.shape[1] // HEAD
    heads = jax.ShapeDtypeStruct((g, tokens, HEAD), LOW)
    block, *_, ssem, rsem = gather_scratch(BLOCK, d)
    cols = g * QUERIES
    return pl.pallas_call(
        _project, in_specs=[HBM] * 7, out_specs=[HBM] * 7, out_shape=[states, heads, one, one, states, heads, jax.ShapeDtypeStruct((g, tokens), jnp.float32)],
        scratch_shapes=[*gather_scratch(tokens, d), *(pltpu.VMEM(w.shape, LOW) for w in (wq, wk, wv)), pltpu.SemaphoreType.DMA((3,)), block, ssem, rsem,
                        pltpu.VMEM((1, cols), jnp.float32), pltpu.VMEM((HEAD + SUM_ROWS, cols), jnp.float32), pltpu.VMEM((KEYS, cols), jnp.int32)],
        compiler_params=pltpu.CompilerParams(collective_id=0, has_side_effects=True, vmem_limit_bytes=ALL_VMEM), cost_estimate=work(70, 60), name="project",
    )(own, dy, wq, wk, wv, cos, sin)


NARROW = 256


def _hidden(own_ref, by_hidden_ref, wg_ref, wu_ref, all_ref, hidden_ref, by_gate_ref, by_up_ref, store, local, kept, ssem, rsem, wg, wu, wsem):
    gather = Gather(own_ref, all_ref, (ssem, rsem), local, store, kept)
    tiles = wg.shape[0]

    def weights(n):
        cut = pl.ds(pl.multiple_of(n * NARROW, NARROW), NARROW)
        return [pltpu.make_async_copy(a.at[:, cut], b.at[n], wsem.at[i, n]) for i, (a, b) in enumerate(((wg_ref, wg), (wu_ref, wu)))]

    gather.begin()
    loop(0, tiles, lambda n: [copy.start() for copy in weights(n)] and None)

    def group(k):
        gather.arrive(k)

        def body(*refs):
            bys, hiddens, by_gates, by_ups = (refs[n * GROUPS : (n + 1) * GROUPS] for n in range(4))
            j = pl.program_id(0)

            @pl.when(k == 0)
            def _():
                for copy in weights(j):
                    copy.wait()

            t = gather.states(k)
            gate, up = _nn(t, wg[j]), _nn(t, wu[j])
            for i in range(GROUPS):
                rows = slice(i * HALF, (i + 1) * HALF)
                g, u, by = gate[rows], up[rows], bys[i][...].astype(jnp.float32)
                s = jax.nn.sigmoid(g)
                silu = g * s
                hiddens[i][...] = (silu * u).astype(LOW)
                by_ups[i][...] = (by * silu).astype(LOW)
                by_gates[i][...] = (by * u * (s + silu * (1 - s))).astype(LOW)

        piece = [pl.BlockSpec((HALF, NARROW), lambda j, at=gather.rows(k, i): (at, j)) for i in range(GROUPS)]
        pltpu.emit_pipeline(body, grid=(tiles,), in_specs=piece, out_specs=piece * 3)(
            *(ref for ref in (by_hidden_ref, hidden_ref, by_gate_ref, by_up_ref) for _ in range(GROUPS)))

    loop(0, GROUPS, group)
    gather.end()


def hidden_units(own, by_hidden, w_gate, w_up):
    tokens, units = by_hidden.shape
    d = own.shape[1]
    part = jax.ShapeDtypeStruct((tokens, units), LOW)
    kept = pltpu.VMEM((units // NARROW, d, NARROW), LOW)
    return pl.pallas_call(
        _hidden, in_specs=[HBM] * 4, out_specs=[HBM] * 4, out_shape=[jax.ShapeDtypeStruct((tokens, d), LOW), part, part, part],
        scratch_shapes=[*gather_scratch(tokens, d), kept, kept, pltpu.SemaphoreType.DMA((2, units // NARROW))],
        compiler_params=pltpu.CompilerParams(collective_id=1, has_side_effects=True, vmem_limit_bytes=ALL_VMEM),
        cost_estimate=work(90, 200), name="hidden_units",
    )(own, by_hidden, w_gate, w_up)


ACROSS, ALONG_X, ALONG_Y, OWN = range(4)
SLICES = 8
HALVES = 2


def _unit(u):
    part = lax.div(u, 4)
    middle = (part >= 2) & (part < 6)
    odd = lax.rem(part, 2)
    chip = jnp.where(middle, 1 + odd, jnp.where(part < 2, ACROSS, OWN))
    half = jnp.where(middle, lax.rem(odd + lax.div(part, 4), 2), odd)
    return chip, 4 * half + lax.rem(u, 4)


def _reduce(take, fillers, finish, counts, *refs):
    groups = []
    for count in counts:
        groups.append(refs[:count])
        refs = refs[count:]
    a_refs, w_refs, extra_refs, fill_refs, out_refs, fill_outs, a_bufs, w_bufs = groups
    mine, theirs, far, along, passed, asem, wsem, esem, osem, ssem, rsem = refs
    slices = mine.shape[0]
    half = slices // 2
    me, (x, y, c), (dx, dy, dc) = place()
    nt = [w.shape[1] == SLICE and w_ref.shape[0] == slices * SLICE for w, w_ref in zip(w_bufs, w_refs)]
    cut = lambda n: pl.ds(pl.multiple_of(n * SLICE, SLICE), SLICE)

    def weight(i, n):
        return pltpu.make_async_copy(w_refs[i].at[cut(n)] if nt[i] else w_refs[i].at[:, cut(n)], w_bufs[i].at[n], wsem.at[i, n])

    chips = (dx + 2 * (1 - 2 * y), dx, dy, me)

    def load(m):
        copies = []
        for s, device in enumerate((chips[m], chips[m] + 1 - 2 * c)):
            for i, (ref, buf) in enumerate(zip(a_refs, a_bufs)):
                at = pl.ds(s * BLOCK, BLOCK)
                copies.append(pltpu.make_async_copy(ref.at[:, rows_of(device)], buf.at[m % 2, :, at], asem.at[m % 2, i, s]) if len(ref.shape) == 3 else
                              pltpu.make_async_copy(ref.at[rows_of(device)], buf.at[m % 2, at], asem.at[m % 2, i, s]))
        return copies

    def begin(copies):
        for copy in copies:
            copy.start()

    def finished(copies):
        for copy in copies:
            copy.wait()

    halves = (pl.ds(0, half), pl.ds(half, half))
    sems = (ssem, rsem)
    n_far = 2 * slices
    core_slice = lambda n: send(mine.at[n], theirs.at[ACROSS, n], sems, n, dc)
    far_slice = lambda n: send(passed.at[ACROSS, n], far.at[n], sems, slices + n, jnp.where(n < half, dx, dy))
    to_core, to_near = {}, {}
    for m in (ALONG_X, ALONG_Y, OWN):
        for h, at in enumerate(halves):
            to_core[m, h] = send(mine.at[at], theirs.at[m, at], sems, n_far + 4 * m + h, dc)
            if m != OWN:
                to_near[m, h] = send(passed.at[m, at], along.at[m - 1, at], sems, n_far + 4 * m + 2 + h, (dx, dy)[m - 1])

    begin(load(ACROSS))
    loop(0, slices, lambda n: begin([weight(i, n) for i in range(len(w_refs))]))
    begin(load(ALONG_X))
    greet((dx, dy, dc))

    def add(m, n, *terms):
        passed[m, n] = sum((t.astype(jnp.float32) for t in terms), passed[m, n].astype(jnp.float32)).astype(LOW)

    def join(m, h, by_far=False):
        to_core[m, h].wait_recv()

        def one(i):
            n = h * half + i
            if by_far:
                far_slice(n).wait_recv()
                add(m, n, theirs[m, n], far[n])
            else:
                add(m, n, theirs[m, n])

        loop(0, half, one)
        to_near[m, h].start()

    def join_far(n):
        core_slice(n).wait_recv()
        add(ACROSS, n, theirs[ACROSS, n])
        far_slice(n).start()

    left = lambda h: loop(h * half, (h + 1) * half, lambda n: core_slice(n).wait_send())
    part = 4
    first = {0: [lambda: finished(load(ACROSS))], 2: [lambda: left(0), lambda: finished(load(ALONG_X)), lambda: begin(load(ALONG_Y))],
             3: [lambda: left(1), lambda: finished(load(ALONG_Y))], 4: [to_core[ALONG_Y, 1].wait_send],
             5: [to_core[ALONG_X, 0].wait_send, lambda: begin(load(OWN)), *(functools.partial(f, fill_refs, fill_outs) for f in fillers[:1])],
             6: [to_core[ALONG_Y, 0].wait_send, lambda: finished(load(OWN))], 7: [to_core[ALONG_X, 1].wait_send]}
    done = [(ALONG_X, 0), (ALONG_Y, 1), (ALONG_X, 1), (ALONG_Y, 0)]

    def unit(u):
        m, n = _unit(u)
        slot = lax.rem(m, 2)
        for at, acts in first.items():

            @pl.when(u == at * part)
            def _(acts=acts):
                for act in acts:
                    act()

        @pl.when(u < slices)
        def _():
            finished([weight(i, n) for i in range(len(w_refs))])

        acc = sum(_dot(t, w[n], 1, 1 if t_ else 0) for t, w, t_ in zip(take([b.at[slot] for b in a_bufs]), w_bufs, nt)).astype(LOW)
        passed[m, n] = acc[:BLOCK]
        mine[n] = acc[BLOCK:]
        pl.when(u < slices)(lambda: core_slice(u).start())
        pl.when((u > 0) & (u <= slices))(lambda: join_far(u - 1))
        for i, (chip, h) in enumerate(done):
            pl.when(u == (i + 3) * part - 1)(to_core[chip, h].start)
            pl.when(u == (i + 3) * part + 1)(functools.partial(join, chip, h, i >= 2))
        for h in range(HALVES):
            pl.when(u == (h + 7) * part - 1)(to_core[OWN, h].start)

    loop(0, part * 8, unit)
    for fill in fillers[1:]:
        fill(fill_refs, fill_outs)

    last = [to_core[OWN, h] for h in range(HALVES)]
    for copy in last:
        copy.wait_send()
    loop(0, slices, lambda n: far_slice(n).wait_send())
    extras = [passed.at[ACROSS], mine][: len(extra_refs)]
    slice_copies = lambda pairs, sem, n: [pltpu.make_async_copy(r.at[:, cut(n)], b.at[n], sem.at[i, n]) for i, (r, b) in enumerate(pairs)]
    loads = list(zip(extra_refs, extras))
    loop(0, slices, lambda n: begin(slice_copies(loads, esem, n)))
    loop(0, slices, lambda n: finished(slice_copies(loads, esem, n)))
    for copy in to_near.values():
        copy.wait_send()
    for copy in (*last, *to_near.values()):
        copy.wait_recv()

    def sum_of(n):
        return sum(t.astype(jnp.float32) for t in (passed[OWN, n], theirs[OWN, n], along[0, n], along[1, n]))

    results = finish(slices, sum_of, extras, theirs.at[ACROSS])

    def put(n):
        return [pltpu.make_async_copy(b.at[n], r.at[:, cut(n)], osem.at[i, n]) for i, (r, b) in enumerate(zip(out_refs, results))]

    loop(0, slices, lambda n: begin(put(n)))
    loop(0, slices, lambda n: finished(put(n)))


def reduce(name, number, take, terms, weights, extras, outs, finish, gflops, fillers=(), fill=(), fill_outs=()):
    d = extras[0].shape[1]
    slices = d // SLICE
    state = (slices, BLOCK, SLICE)
    both = 2 * BLOCK
    blocks = [(2, t.shape[0], both, t.shape[2]) if t.ndim == 3 else (2, both, t.shape[1]) for t in terms]
    kept = [(slices, SLICE, w.shape[1]) if w.shape[0] == d else (slices, w.shape[0], SLICE) for w in weights]
    dma = pltpu.SemaphoreType.DMA
    counts = (len(terms), len(weights), len(extras), len(fill), outs, len(fill_outs), len(terms), len(weights))
    low = lambda *shape: pltpu.VMEM(shape, LOW)
    return pl.pallas_call(
        functools.partial(_reduce, take, fillers, finish, counts),
        in_specs=[HBM] * sum(counts[:4]), out_specs=[HBM] * (outs + len(fill_outs)),
        out_shape=[jax.ShapeDtypeStruct((BLOCK, d), LOW)] * outs + [jax.ShapeDtypeStruct(s, LOW) for s in fill_outs],
        scratch_shapes=[*(low(*s) for s in blocks), *(low(*s) for s in kept), low(*state), low(4, *state), low(*state), low(2, *state), low(4, *state),
                        dma((2, len(terms), 2)), dma((len(weights), slices)), dma((len(extras), slices)), dma((outs, slices)), dma((32,)), dma((32,))],
        compiler_params=pltpu.CompilerParams(collective_id=number, has_side_effects=True, vmem_limit_bytes=ALL_VMEM),
        cost_estimate=work(gflops, 60), name=name,
    )(*terms, *weights, *extras, *fill)


def finish_norm(slices, sum_of, extras, spare):
    (states,) = extras

    def one(n, squares):
        h = (states[n].astype(jnp.float32) + sum_of(n)).astype(LOW)
        states[n] = h
        wide = h.astype(jnp.float32)
        return squares + jnp.sum(wide * wide, -1, keepdims=True)

    squares = lax.fori_loop(0, slices, one, jnp.zeros((BLOCK, 1), jnp.float32))
    scale = lax.rsqrt(squares / (slices * SLICE) + EPS)

    def two(n):
        spare[n] = (states[n].astype(jnp.float32) * scale).astype(LOW)

    loop(0, slices, two)
    return states, spare


def finish_back(slices, sum_of, extras, spare):
    states, rest = extras

    def one(n, so_far):
        squares, across = so_far
        h, g = states[n].astype(jnp.float32), sum_of(n)
        return squares + jnp.sum(h * h, -1, keepdims=True), across + jnp.sum(h * g, -1, keepdims=True)

    zero = jnp.zeros((BLOCK, 1), jnp.float32)
    squares, across = lax.fori_loop(0, slices, one, (zero, zero))
    size = slices * SLICE
    scale = lax.rsqrt(squares / size + EPS)
    back = scale * scale * scale * (across / size)

    def two(n):
        by = sum_of(n) * scale - states[n].astype(jnp.float32) * back
        rest[n] = (rest[n].astype(jnp.float32) + by).astype(LOW)

    loop(0, slices, two)
    return (rest,)


def side_by_side(r):
    return jnp.concatenate([r[n] for n in range(r.shape[0])], axis=1)


def heads_side_by_side(refs):
    return [side_by_side(refs[0])]


def as_they_are(refs):
    return [r[...] for r in refs]


def heads_and_two(refs):
    q, k, v = refs
    return [side_by_side(q), k[...], v[...]]


WIDE = 512


def fill_by_hidden(part, refs, outs):
    dy_ref, wd_ref = refs
    (units, d), tokens = wd_ref.shape, dy_ref.shape[0]
    rows, wide = tokens // 2, units // 4

    def body(dy, w, out):
        out[...] = _nt(dy[...], w[...]).astype(LOW)

    pltpu.emit_pipeline(body, grid=(units // wide,), in_specs=[pl.BlockSpec((rows, d), lambda j: (part, 0)), pl.BlockSpec((wide, d), lambda j: (j, 0))],
                        out_specs=[pl.BlockSpec((rows, wide), lambda j: (part, j))])(dy_ref, wd_ref, outs[0])


def fill_by_wo(refs, outs):
    heads_ref, all_h_ref = refs[:2]
    g, tokens, _ = heads_ref.shape

    def body(heads, h, out):
        out[...] = _tn(side_by_side(heads), h[...]).astype(LOW)

    pltpu.emit_pipeline(body, grid=(all_h_ref.shape[1] // WIDE,), in_specs=[pl.BlockSpec((g, tokens, HEAD), lambda j: (0, 0, 0)),
                                                                          pl.BlockSpec((tokens, WIDE), lambda j: (0, j))],
                        out_specs=[pl.BlockSpec((g * HEAD, WIDE), lambda j: (0, j))])(heads_ref, all_h_ref, outs[0])


def fill_by_rest(refs, outs):
    a_ref, q_ref, k_ref, v_ref = refs[2:]
    g, tokens, _ = q_ref.shape
    one = pl.BlockSpec((tokens, HEAD), lambda j: (0, 0))
    narrow = pl.BlockSpec((WIDE, HEAD), lambda j: (j, 0))

    def body(a, q, k, v, by_q, by_k, by_v):
        t = _tn(a[...], jnp.concatenate([side_by_side(q), k[...], v[...]], axis=1)).astype(LOW)
        by_q[...], by_k[...], by_v[...] = t[:, : g * HEAD], t[:, g * HEAD : (g + 1) * HEAD], t[:, (g + 1) * HEAD :]

    pltpu.emit_pipeline(body, grid=(a_ref.shape[1] // WIDE,),
                        in_specs=[pl.BlockSpec((tokens, WIDE), lambda j: (0, j)), pl.BlockSpec((g, tokens, HEAD), lambda j: (0, 0, 0)), one, one],
                        out_specs=[pl.BlockSpec((WIDE, g * HEAD), lambda j: (j, 0)), narrow, narrow])(a_ref, q_ref, k_ref, v_ref, *outs[1:])


def _by_heads(h, wo, heads, out, delta):
    t = _nt(h[...], wo[...]).astype(LOW)
    for n in range(out.shape[0]):
        part = t[:, n * HEAD : (n + 1) * HEAD]
        out[n] = part
        delta[n : n + 1, :] = (part.astype(jnp.float32) * heads[n].astype(jnp.float32)).T.sum(axis=0, keepdims=True)


def by_heads(all_h, wo, heads):
    g, tokens, _ = heads.shape
    d = wo.shape[1]
    rows = WIDE
    tile = pl.BlockSpec((g, rows, HEAD), lambda i: (0, i, 0))
    return pl.pallas_call(
        _by_heads, grid=(tokens // rows,), in_specs=[pl.BlockSpec((rows, d), lambda i: (i, 0)), pl.BlockSpec(wo.shape, lambda i: (0, 0)), tile],
        out_specs=[tile, pl.BlockSpec((g, rows), lambda i: (0, i))],
        out_shape=[jax.ShapeDtypeStruct(heads.shape, LOW), jax.ShapeDtypeStruct((g, tokens), jnp.float32)],
        compiler_params=pltpu.CompilerParams(dimension_semantics=("arbitrary",), vmem_limit_bytes=VMEM), cost_estimate=work(9, 24), name="by_heads",
    )(all_h, wo, heads)


def mm(eq, a, b):
    return jnp.einsum(eq, a, b, preferred_element_type=jnp.float32).astype(LOW)


def layer(x, dy, w):
    tokens, d = BLOCK * 8, x.shape[1]
    cos, sin = angles(tokens)
    a, q, k, v, all_dy, heads, lse = project(x, dy, w["wq"], w["wk"], w["wv"], cos, sin)
    units = w["w_down"].shape[0]
    h, b_own, by_hidden = reduce("add_heads", 2, heads_side_by_side, [heads], [w["wo"]], [x], 2, finish_norm, 60,
                                 [functools.partial(fill_by_hidden, part) for part in range(2)], [all_dy, w["w_down"]], [(tokens, units)])
    b, hidden, by_gate, by_up = hidden_units(b_own, by_hidden, w["w_gate"], w["w_up"])
    (by_h,) = reduce("by_states", 3, as_they_are, [by_gate, by_up], [w["w_gate"], w["w_up"]], [h, dy], 1, finish_back, 80)
    all_h = lax.all_gather(by_h, "tp", axis=0, tiled=True)
    by_w = {"w_down": mm("tu,td->ud", hidden, all_dy), "w_gate": mm("td,tu->du", b, by_gate), "w_up": mm("td,tu->du", b, by_up)}
    by_out, delta = by_heads(all_h, w["wo"], heads)
    by_q, by_k, by_v = attend_bwd(q, k, v, by_out, lse, delta, cos, sin)
    by_x, *rest = reduce("by_input", 4, heads_and_two, [by_q, by_k, by_v], [w["wq"], w["wk"], w["wv"]], [x, by_h], 1, finish_back, 60,
                         [fill_by_wo, fill_by_rest], [heads, all_h, a, by_q, by_k, by_v], [w[name].shape for name in ("wo", "wq", "wk", "wv")])
    by_w.update(zip(("wo", "wq", "wk", "wv"), rest))
    return by_x, by_w


def solution(mesh):
    def step(x, dy, *weights):
        by_x, by_w = layer(x[0], dy[0], dict(zip(NAMES, weights, strict=True)))
        return (by_x[None], *(by_w[name] for name in NAMES))

    states, by_columns, by_rows = P("dp", "tp", None), P(None, "tp"), P("tp", None)
    weights = (by_columns, by_columns, by_columns, by_rows, by_columns, by_columns, by_rows)
    own = tuple(P("dp", "tp") if spec == by_columns else P(("dp", "tp"), None) for spec in weights)
    return jax.shard_map(step, mesh=mesh, in_specs=(states, states, *weights), out_specs=(states, *own), check_vma=False)
```

```python
import functools

import jax
import jax.numpy as jnp
import numpy as np
from jax import lax
from jax.experimental import pallas as pl
from jax.experimental.pallas import tpu as pltpu
from jax.sharding import PartitionSpec as P

NEG = -1e30
HIDDEN = 2 * NEG
LOG2E = 1.4426950408889634
MIB = 2**20
VMEM, ALL_VMEM = 56 * MIB, 63 * MIB
STRIP = 512
KEYS = 512
QUERIES, QUERIES_BACK = 1024, 512
HEAD = 128
SUM_ROWS = 8
SCALE = HEAD**-0.5
E = SCALE * LOG2E


def _dot(a, b, ca, cb):
    return lax.dot_general(a, b, (((ca,), (cb,)), ((), ())), preferred_element_type=jnp.float32)


_nn, _nt, _tn = (functools.partial(_dot, ca=ca, cb=cb) for ca, cb in ((1, 0), (1, 1), (0, 0)))


def work(gflops, megabytes):
    return pl.CostEstimate(flops=gflops * 10**9, bytes_accessed=megabytes * 10**6, transcendentals=0)


def _seen(iq, bq):
    first = iq * bq
    return lax.div(first + 1, KEYS), lax.div(first + bq - 1 + KEYS, KEYS)


def _gap(cols, bq):
    return lax.rem(lax.broadcasted_iota(jnp.int32, (KEYS, cols), 1), bq) - lax.broadcasted_iota(jnp.int32, (KEYS, cols), 0)


def _row(ref):
    return jnp.concatenate([ref[n : n + 1, :] for n in range(ref.shape[0])], axis=1)


def _forward(q_ref, k_ref, v_ref, o_ref, lse_ref, top_s, mix_s, gap_s):
    g, bq, d = q_ref.shape
    cols = g * bq
    iq = pl.program_id(0)
    strips = range(0, cols, STRIP)
    gap_s[...] = _gap(cols, bq)
    top_s[...] = jnp.full_like(top_s, NEG)
    mix_s[...] = jnp.zeros_like(mix_s)
    ones = jnp.ones((SUM_ROWS, KEYS), k_ref.dtype)

    def block(j, masked):
        here = pl.ds(j * KEYS, KEYS)
        scores = [_nt(k_ref[here, :], q_ref[...].reshape(cols, d)[at : at + STRIP, :]) for at in strips]
        weights, keeps = [], []
        for at, s in zip(strips, scores):
            if masked:
                s = jnp.where(gap_s[:, at : at + STRIP] >= j * KEYS - iq * bq, s, HIDDEN)
            old = top_s[:, at : at + STRIP]
            top = jnp.maximum(old, s.max(axis=0, keepdims=True))
            top_s[:, at : at + STRIP] = top
            weights.append(jnp.exp2((s - top) * E).astype(k_ref.dtype))
            keeps.append(jnp.exp2((old - top) * E))
        for at, p, keep in zip(strips, weights, keeps):
            values = jnp.concatenate([v_ref[here, :].T, ones], axis=0)
            mix_s[:, at : at + STRIP] = mix_s[:, at : at + STRIP] * keep + _nn(values, p)

    whole, last = _seen(iq, bq)
    loop(0, whole, lambda j: block(j, False))
    loop(whole, last, lambda j: block(j, True))
    total = mix_s[d : d + 1, :]
    o_ref[...] = (mix_s[:d, :] * (1 / total)).T.reshape(g, bq, d).astype(o_ref.dtype)
    lse = top_s[...] * SCALE + jnp.log(total)
    for n in range(g):
        lse_ref[n : n + 1, :] = lse[:, n * bq : (n + 1) * bq]


def _cost(q, width):
    g, s, d = q.shape
    return pl.CostEstimate(flops=2 * g * s * s * width, transcendentals=g * s * s, bytes_accessed=4 * q.size * q.dtype.itemsize)


def _backward(q_ref, k_ref, v_ref, do_ref, lse_ref, delta_ref, cos_ref, sin_ref, dq_ref, dk_ref, dv_ref, dq_s, dk_s, dv_s, gap_s):
    g, bq, d = q_ref.shape
    cols, low = g * bq, q_ref.dtype
    iq = pl.program_id(0)
    strips = range(0, cols, STRIP)

    @pl.when(iq == 0)
    def _():
        gap_s[...] = _gap(cols, bq)
        dk_s[...] = jnp.zeros_like(dk_s)
        dv_s[...] = jnp.zeros_like(dv_s)

    dq_s[...] = jnp.zeros_like(dq_s)
    lses, deltas = _row(lse_ref) * LOG2E, _row(delta_ref)

    def block(j, masked):
        here = pl.ds(j * KEYS, KEYS)
        qs = [q_ref[...].reshape(cols, d)[at : at + STRIP, :] for at in strips]
        dos = [do_ref[...].reshape(cols, d)[at : at + STRIP, :] for at in strips]
        scores = [_nt(k_ref[here, :], x) for x in qs]
        dps = [_nt(v_ref[here, :], x) for x in dos]
        for n, at in enumerate(strips):
            p = jnp.exp2(scores[n] * E - lses[:, at : at + STRIP])
            if masked:
                p = jnp.where(gap_s[:, at : at + STRIP] >= j * KEYS - iq * bq, p, 0.0)
            ds = (p * (dps[n] - deltas[:, at : at + STRIP])).astype(low)
            dv_s[here, :] += _nn(p.astype(low), dos[n])
            dk_s[here, :] += _nn(ds, qs[n])
            dq_s[:, at : at + STRIP] += _nn(k_ref[here, :].T, ds)

    whole, last = _seen(iq, bq)
    loop(0, whole, lambda j: block(j, False))
    loop(whole, last, lambda j: block(j, True))
    here = pl.ds(iq * bq, bq)
    by_q = (dq_s[...] * SCALE).T
    cos, sin = cos_ref[here, :], sin_ref[here, :]
    for n in range(g):
        dq_ref[n] = turn(by_q[n * bq : (n + 1) * bq, :], cos, -sin)

    @pl.when(iq == pl.num_programs(0) - 1)
    def _():
        dk_ref[...] = turn(dk_s[...] * SCALE, cos_ref[...], -sin_ref[...])
        dv_ref[...] = dv_s[...].astype(dv_ref.dtype)


def attend_bwd(q, k, v, d_out, lse, delta, cos, sin):
    g, s, d = q.shape
    bq = QUERIES_BACK
    queries = pl.BlockSpec((g, bq, d), lambda i: (0, i, 0))
    keys = pl.BlockSpec((s, d), lambda i: (0, 0))
    table = pl.BlockSpec(cos.shape, lambda i: (0, 0))
    stats = pl.BlockSpec((g, bq), lambda i: (0, i))
    return pl.pallas_call(
        _backward, grid=(s // bq,), in_specs=[queries, keys, keys, queries, stats, stats, table, table], out_specs=[queries, keys, keys],
        scratch_shapes=[pltpu.VMEM((d, g * bq), jnp.float32), pltpu.VMEM((s, d), jnp.float32), pltpu.VMEM((s, d), jnp.float32),
                        pltpu.VMEM((KEYS, g * bq), jnp.int32)],
        out_shape=[jax.ShapeDtypeStruct(t.shape, t.dtype) for t in (q, k, v)],
        compiler_params=pltpu.CompilerParams(dimension_semantics=("arbitrary",), vmem_limit_bytes=VMEM), cost_estimate=_cost(q, 5 * d), name="attend_bwd",
    )(q, k, v, d_out, lse, delta, cos, sin)


THETA = 10000
NAMES = ("wq", "wk", "wv", "wo", "w_gate", "w_up", "w_down")
EPS = 1e-6
LOW = jnp.bfloat16
BLOCK = 256
SLICE = 512
HBM = pl.BlockSpec(memory_space=pltpu.HBM)


def normed(h):
    wide = h.astype(jnp.float32)
    scale = lax.rsqrt(jnp.mean(wide**2, -1, keepdims=True) + EPS)
    return (wide * scale).astype(jnp.bfloat16)


def place():
    me = lax.axis_index("tp")
    x, y, c = lax.div(me, 4), lax.rem(lax.div(me, 2), 2), lax.rem(me, 2)
    return me, (x, y, c), (me + 4 * (1 - 2 * x), me + 2 * (1 - 2 * y), me + 1 - 2 * c)


def greet(neighbours):
    barrier = pltpu.get_barrier_semaphore()
    for device in neighbours:
        pl.semaphore_signal(barrier, inc=1, device_id={"tp": device}, device_id_type=pl.DeviceIdType.MESH)
    pl.semaphore_wait(barrier, len(neighbours))


def send(src, dst, sems, n, device):
    return pltpu.make_async_remote_copy(src_ref=src, dst_ref=dst, send_sem=sems[0].at[n], recv_sem=sems[1].at[n], device_id={"tp": device},
                                        device_id_type=pl.DeviceIdType.MESH)


def rows_of(device, half=None):
    if half is None:
        return pl.ds(pl.multiple_of(device * BLOCK, BLOCK), BLOCK)
    return pl.ds(pl.multiple_of(device * BLOCK + half * (BLOCK // 2), BLOCK // 2), BLOCK // 2)


def loop(start, end, f):
    def step(i, _):
        f(i)

    lax.fori_loop(start, end, step, None)


HALF = BLOCK // 2
CHIP = 2 * BLOCK
GROUPS = 4


WAYS = [[[int(n) for n in way.split("-")] for way in ways.split()] for ways in ("0", "3-5-8 1-6-7 7 8", "2-9 4-10 9 10", "5-11 6-12 11 12")]


class Gather:
    def __init__(self, own_ref, all_ref, sems, local, store=None, kept=None):
        self.own_ref, self.all_ref, self.store, self.local, self.kept = own_ref, all_ref, store, local, kept
        me, (x, y, c), (dx, dy, dc) = place()
        self.at, self.near = (x, y, c), (dx, dy, dc)
        if store is None:
            half = lambda device, n: all_ref.at[pl.ds(pl.multiple_of(device * BLOCK + n * HALF, HALF), HALF)]
            self.own = own_ref
            mine = [own_ref.at[pl.ds(n * HALF, HALF)] for n in range(2)]
            x1, x2, y1, y2, d0, d1 = half(me, 1), half(me, 0), half(me, 0), half(me, 1), half(dy, 0), half(dx, 1)
            own, came = all_ref.at[rows_of(me)], [half(dx, 1), half(dy, 0), half(dx, 0), half(dy, 1)]
            came += [half(dx + 2 * (1 - 2 * y), n) for n in range(2)]
        else:
            slot = lambda group, i, n=1: store.at[pl.ds(pl.multiple_of(group * CHIP + i * HALF, HALF), n * HALF)]
            own = self.own = slot(0, 2 * c, 2)
            mine = (slot(0, 2 * c), slot(0, 2 * c + 1))
            came = x1, y1, x2, y2, d0, d1 = [slot(g, i) for g, i in ((1, c), (1, 2 + c), (2, c), (2, 2 + c), (3, 2 * c), (3, 2 * c + 1))]
        steps = [(self.own, own, dc), (mine[1], x1, dx), (mine[0], x2, dx), (mine[0], y1, dy), (mine[1], y2, dy), (came[1], d0, dx), (came[0], d1, dy),
                 *((t, t, dc) for t in came)]
        self.copies = [send(a, b, sems, n, to) for n, (a, b, to) in enumerate(steps)]

    def begin(self, change=None):
        load = pltpu.make_async_copy(self.own_ref, self.own, self.local.at[0])
        load.start()
        load.wait()
        if change is not None:
            rows = 32

            def some(n):
                here = pl.ds(pl.multiple_of(2 * HALF * self.at[2] + n * rows, rows), rows)
                self.store[here, :] = change(self.store[here, :])

            loop(0, BLOCK // rows, some)
        greet(self.near)
        self.start()

    def start(self):
        for n in (1, 3, 2, 4, 0):
            self.copies[n].start()

    def arrive(self, group):
        for k in range(GROUPS):
            pl.when(group == k)(functools.partial(self.take, k))
        for i in range(GROUPS):
            self.keep(group, i).start()

    def take(self, group):
        for n, *onward in WAYS[group]:
            self.copies[n].wait_recv()
            for m in onward:
                self.copies[m].start()

    def rows(self, group, i):
        x, y, c = self.at
        mixed = (group == 1) | (group == 2)
        turn_x = jnp.where(mixed, 1 if i < 2 else 0, lax.div(group, 3))
        turn_y = jnp.where(mixed, 0 if i < 2 else 1, lax.div(group, 3))
        core = jnp.where(mixed, i % 2, i // 2)
        half = jnp.where(mixed, 2 - group if i < 2 else group - 1, i % 2)
        device = (x + turn_x * (1 - 2 * x)) * 4 + (y + turn_y * (1 - 2 * y)) * 2 + core
        return device * 2 + half

    def keep(self, group, i):
        here = pl.ds(pl.multiple_of(group * CHIP + i * HALF, HALF), HALF)
        there = pl.ds(pl.multiple_of(self.rows(group, i) * HALF, HALF), HALF)
        return pltpu.make_async_copy(self.store.at[here], self.all_ref.at[there], self.kept.at[group, i])

    def states(self, group):
        return self.store[pl.ds(pl.multiple_of(group * CHIP, CHIP), CHIP), :]

    def end(self):
        def some(group):
            for i in range(GROUPS):
                self.keep(group, i).wait()

        if self.store is not None:
            loop(0, GROUPS, some)
        for copy in self.copies:
            copy.wait_send()


def gather_scratch(tokens, d):
    dma = pltpu.SemaphoreType.DMA
    return [pltpu.VMEM((tokens, d), LOW), dma((1,)), dma((GROUPS, GROUPS)), dma((13,)), dma((13,))]


def turn(t, cos, sin):
    half = HEAD // 2
    other = jnp.concatenate([t[:, half:], t[:, :half]], axis=1)
    return (t * jnp.concatenate([cos, cos], axis=1) + other * jnp.concatenate([-sin, sin], axis=1)).astype(LOW)


def angles(tokens):
    half = HEAD // 2
    angle = np.arange(tokens, dtype=np.float32)[:, None] * THETA ** (-np.arange(half, dtype=np.float32) / half)
    return jnp.asarray(np.cos(angle), jnp.float32), jnp.asarray(np.sin(angle), jnp.float32)


def _project(own_ref, dy_ref, wq_ref, wk_ref, wv_ref, cos_ref, sin_ref, wg_ref, wu_ref, all_ref, q_ref, k_ref, v_ref, all_dy_ref, o_ref, lse_ref,
             wg_across_ref, wu_across_ref, store, local, kept, ssem, rsem, wq, wk, wv, wsem, block, dy_ssem, dy_rsem, *scratch):
    gather = Gather(own_ref, all_ref, (ssem, rsem), local, store, kept)
    loads = [pltpu.make_async_copy(a, b, wsem.at[n]) for n, (a, b) in enumerate(((wq_ref, wq), (wk_ref, wk), (wv_ref, wv)))]
    for load in loads:
        load.start()
    gather.begin(normed)
    dy = Gather(dy_ref, all_dy_ref, (dy_ssem, dy_rsem), local)
    keep = pltpu.make_async_copy(dy_ref, block, local.at[0])
    keep.start()
    for load in loads:
        load.wait()
    keep.wait()
    keep = pltpu.make_async_copy(block, all_dy_ref.at[rows_of(lax.axis_index("tp"))], local.at[0])
    keep.start()

    def group(k):
        gather.arrive(k)
        pl.when(k == 1)(dy.start)

        def body(*refs):
            coses, sins, qs, ks, vs = (refs[n * GROUPS : (n + 1) * GROUPS] for n in range(5))
            t = gather.states(k)
            by_q, by_k, by_v = (_nn(t, w[...]).astype(LOW).astype(jnp.float32) for w in (wq, wk, wv))
            for i in range(GROUPS):
                rows = slice(i * HALF, (i + 1) * HALF)
                cos, sin = coses[i][...], sins[i][...]
                for n in range(q_ref.shape[0]):
                    qs[i][n] = turn(by_q[rows, n * HEAD : (n + 1) * HEAD], cos, sin)
                ks[i][...] = turn(by_k[rows], cos, sin)
                vs[i][...] = by_v[rows].astype(LOW)

        heads, one, table = [], [], []
        for i in range(GROUPS):
            at = gather.rows(k, i)
            heads.append(pl.BlockSpec((q_ref.shape[0], HALF, HEAD), lambda j, at=at: (0, at, 0)))
            one.append(pl.BlockSpec((HALF, HEAD), lambda j, at=at: (at, 0)))
            table.append(pl.BlockSpec((HALF, cos_ref.shape[1]), lambda j, at=at: (at, 0)))
        pltpu.emit_pipeline(body, grid=(1,), in_specs=[*table, *table], out_specs=[*heads, *one, *one])(
            *(ref for ref in (cos_ref, sin_ref, q_ref, k_ref, v_ref) for _ in range(GROUPS)))

    loop(0, GROUPS, group)
    g, tokens, d = q_ref.shape
    queries = pl.BlockSpec((g, QUERIES, d), lambda i: (0, i, 0))
    keys = pl.BlockSpec((tokens, d), lambda i: (0, 0))
    pltpu.emit_pipeline(lambda *refs: _forward(*refs, *scratch), grid=(tokens // QUERIES,), in_specs=[queries, keys, keys],
                        out_specs=[queries, pl.BlockSpec((g, QUERIES), lambda i: (0, i))])(q_ref, k_ref, v_ref, o_ref, lse_ref)
    dy.take(0)
    dy.take(1)

    def lay(*refs):
        for a, b in zip(refs[:2], refs[2:]):
            b[...] = a[...].T

    d, units = wg_ref.shape
    tall, flat = pl.BlockSpec((BLOCK, units), lambda i: (i, 0)), pl.BlockSpec((units, BLOCK), lambda i: (0, i))
    pltpu.emit_pipeline(lay, grid=(d // BLOCK,), in_specs=[tall] * 2, out_specs=[flat] * 2)(wg_ref, wu_ref, wg_across_ref, wu_across_ref)
    dy.take(2)
    dy.take(3)
    keep.wait()
    dy.end()
    gather.end()


def project(own, dy, wq, wk, wv, cos, sin, w_gate, w_up):
    d, tokens = own.shape[1], cos.shape[0]
    one, states = jax.ShapeDtypeStruct((tokens, HEAD), LOW), jax.ShapeDtypeStruct((tokens, d), LOW)
    g = wq.shape[1] // HEAD
    heads = jax.ShapeDtypeStruct((g, tokens, HEAD), LOW)
    block, *_, ssem, rsem = gather_scratch(BLOCK, d)
    cols = g * QUERIES
    across = jax.ShapeDtypeStruct(w_gate.shape[::-1], LOW)
    return pl.pallas_call(
        _project, in_specs=[HBM] * 9, out_specs=[HBM] * 9,
        out_shape=[states, heads, one, one, states, heads, jax.ShapeDtypeStruct((g, tokens), jnp.float32), across, across],
        scratch_shapes=[*gather_scratch(tokens, d), *(pltpu.VMEM(w.shape, LOW) for w in (wq, wk, wv)), pltpu.SemaphoreType.DMA((3,)), block, ssem, rsem,
                        pltpu.VMEM((1, cols), jnp.float32), pltpu.VMEM((HEAD + SUM_ROWS, cols), jnp.float32), pltpu.VMEM((KEYS, cols), jnp.int32)],
        compiler_params=pltpu.CompilerParams(collective_id=0, has_side_effects=True, vmem_limit_bytes=ALL_VMEM), cost_estimate=work(70, 60), name="project",
    )(own, dy, wq, wk, wv, cos, sin, w_gate, w_up)


NARROW = 256


def _hidden(own_ref, by_hidden_ref, wg_ref, wu_ref, all_ref, hidden_ref, by_gate_ref, by_up_ref, store, local, kept, ssem, rsem, wg, wu, wsem):
    gather = Gather(own_ref, all_ref, (ssem, rsem), local, store, kept)
    tiles = wg.shape[0]

    def weights(n):
        cut = pl.ds(pl.multiple_of(n * NARROW, NARROW), NARROW)
        return [pltpu.make_async_copy(a.at[:, cut], b.at[n], wsem.at[i, n]) for i, (a, b) in enumerate(((wg_ref, wg), (wu_ref, wu)))]

    gather.begin()
    loop(0, tiles, lambda n: [copy.start() for copy in weights(n)] and None)

    def group(k):
        gather.arrive(k)

        def body(*refs):
            bys, hiddens, by_gates, by_ups = (refs[n * GROUPS : (n + 1) * GROUPS] for n in range(4))
            j = pl.program_id(0)

            @pl.when(k == 0)
            def _():
                for copy in weights(j):
                    copy.wait()

            t = gather.states(k)
            gate, up = _nn(t, wg[j]), _nn(t, wu[j])
            for i in range(GROUPS):
                rows = slice(i * HALF, (i + 1) * HALF)
                g, u, by = gate[rows], up[rows], bys[i][...].astype(jnp.float32)
                s = jax.nn.sigmoid(g)
                silu = g * s
                hiddens[i][...] = (silu * u).astype(LOW)
                by_ups[i][...] = (by * silu).astype(LOW)
                by_gates[i][...] = (by * u * (s + silu * (1 - s))).astype(LOW)

        piece = [pl.BlockSpec((HALF, NARROW), lambda j, at=gather.rows(k, i): (at, j)) for i in range(GROUPS)]
        pltpu.emit_pipeline(body, grid=(tiles,), in_specs=piece, out_specs=piece * 3)(
            *(ref for ref in (by_hidden_ref, hidden_ref, by_gate_ref, by_up_ref) for _ in range(GROUPS)))

    loop(0, GROUPS, group)
    gather.end()


def hidden_units(own, by_hidden, w_gate, w_up):
    tokens, units = by_hidden.shape
    d = own.shape[1]
    part = jax.ShapeDtypeStruct((tokens, units), LOW)
    kept = pltpu.VMEM((units // NARROW, d, NARROW), LOW)
    return pl.pallas_call(
        _hidden, in_specs=[HBM] * 4, out_specs=[HBM] * 4, out_shape=[jax.ShapeDtypeStruct((tokens, d), LOW), part, part, part],
        scratch_shapes=[*gather_scratch(tokens, d), kept, kept, pltpu.SemaphoreType.DMA((2, units // NARROW))],
        compiler_params=pltpu.CompilerParams(collective_id=1, has_side_effects=True, vmem_limit_bytes=ALL_VMEM),
        cost_estimate=work(90, 200), name="hidden_units",
    )(own, by_hidden, w_gate, w_up)


ACROSS, ALONG_X, ALONG_Y, OWN = range(4)
SLICES = 8


def _unit(u):
    part, pair, odd = lax.div(u, SLICES), lax.div(lax.rem(u, SLICES), 2), lax.rem(u, 2)
    chip = jnp.where(part == 0, ACROSS, jnp.where(part == 3, OWN, 1 + odd))
    late = jnp.where(part == 2, 1 - odd, odd)
    return chip, late * (SLICES // 2) + pair


def _reduce(take, fillers, finish, counts, *refs):
    groups = []
    for count in counts:
        groups.append(refs[:count])
        refs = refs[count:]
    a_refs, w_refs, extra_refs, fill_refs, out_refs, fill_outs, a_bufs, (w_buf,) = groups
    mine, theirs, came, passed, asem, wsem, esem, osem, ssem, rsem = refs
    slices = mine.shape[0]
    half = slices // 2
    me, (x, y, c), (dx, dy, dc) = place()
    nt = w_refs[0].shape[0] == slices * SLICE
    cut = lambda n: pl.ds(pl.multiple_of(n * SLICE, SLICE), SLICE)

    def weights(n):
        at, copies = 0, []
        for i, ref in enumerate(w_refs):
            deep = pl.ds(at, ref.shape[nt])
            at += ref.shape[nt]
            pair = (ref.at[cut(n)], w_buf.at[n, :, deep]) if nt else (ref.at[:, cut(n)], w_buf.at[n, deep])
            copies.append(pltpu.make_async_copy(*pair, wsem.at[i, n]))
        return copies

    chips = (dx + 2 * (1 - 2 * y), dx, dy, me)

    def load(m):
        copies = []
        for s, device in enumerate((chips[m], chips[m] + 1 - 2 * c)):
            for i, (ref, buf) in enumerate(zip(a_refs, a_bufs)):
                at = pl.ds(s * BLOCK, BLOCK)
                copies.append(pltpu.make_async_copy(ref.at[:, rows_of(device)], buf.at[m % OWN, :, at], asem.at[m % OWN, i, s]) if len(ref.shape) == 3 else
                              pltpu.make_async_copy(ref.at[rows_of(device)], buf.at[m % OWN, at], asem.at[m % OWN, i, s]))
        return copies

    def begin(copies):
        for copy in copies:
            copy.start()

    def finished(copies):
        for copy in copies:
            copy.wait()

    over = functools.partial(pltpu.make_async_remote_copy, device_id_type=pl.DeviceIdType.MESH)

    def to_core(m, n):
        return over(mine.at[n], theirs.at[m, n], ssem.at[n], rsem.at[m * slices + n], device_id={"tp": dc})

    def to_chip(m, n):
        along_x = (m == ALONG_X) | ((m == ACROSS) & (n < half))
        return over(passed.at[m, n], came.at[m, n], ssem.at[(m + 1) * slices + n], rsem.at[(m + 4) * slices + n], device_id={"tp": jnp.where(along_x, dx, dy)})

    def order(i):
        return lax.rem(i, 2) * half + lax.div(i, 2)

    begin(load(ACROSS))
    loop(0, slices, lambda i: begin(weights(order(i))))
    begin(load(ALONG_X))
    begin(load(ALONG_Y))
    greet((dx, dy, dc))

    def add(m, n, *terms):
        passed[m, n] = sum((t.astype(jnp.float32) for t in terms), passed[m, n].astype(jnp.float32)).astype(LOW)

    def join(u):
        m, n = _unit(u)
        to_core(m, n).wait_recv()
        far = u >= 2 * slices

        @pl.when(far)
        def _():
            to_chip(ACROSS, n).wait_recv()
            add(m, n, theirs[m, n], came[ACROSS, n])

        @pl.when(u < 2 * slices)
        def _():
            add(m, n, theirs[m, n])

        to_chip(m, n).start()

    first = {ACROSS: [lambda: finished(load(ACROSS))], ALONG_X: [lambda: finished(load(ALONG_X) + load(ALONG_Y)), lambda: begin(load(OWN))],
             ALONG_Y: [functools.partial(f, fill_refs, fill_outs) for f in fillers[:1]], OWN: [lambda: finished(load(OWN))]}

    def unit(u):
        m, n = _unit(u)
        for at, acts in first.items():

            @pl.when(u == at * slices)
            def _(acts=acts):
                for act in acts:
                    act()

        @pl.when(u < slices)
        def _():
            finished(weights(n))

        pl.when(u >= slices)(lambda: to_core(m, n).wait_send())
        t = jnp.concatenate(take([b.at[lax.rem(m, OWN)] for b in a_bufs]), axis=1)
        acc = (_nt if nt else _nn)(t, w_buf[n]).astype(LOW)
        passed[m, n] = acc[:BLOCK]
        mine[n] = acc[BLOCK:]
        to_core(m, n).start()
        pl.when((u > 0) & (u <= OWN * slices))(lambda: join(u - 1))

    loop(0, 4 * slices, unit)
    for fill in fillers[1:]:
        fill(fill_refs, fill_outs)

    def gone(n):
        to_core(OWN, n).wait_send()
        to_chip(ACROSS, n).wait_send()

    loop(0, slices, gone)
    extras = [passed.at[ACROSS], mine][: len(extra_refs)]
    slice_copies = lambda pairs, sem, n: [pltpu.make_async_copy(r.at[:, cut(n)], b.at[n], sem.at[i, n]) for i, (r, b) in enumerate(pairs)]
    loads = list(zip(extra_refs, extras))
    loop(0, slices, lambda n: begin(slice_copies(loads, esem, n)))
    loop(0, slices, lambda n: finished(slice_copies(loads, esem, n)))
    def sum_of(n):
        return sum(t.astype(jnp.float32) for t in (passed[OWN, n], theirs[OWN, n], came[ALONG_X, n], came[ALONG_Y, n]))

    def ready(i):
        n = order(i)
        to_core(OWN, n).wait_recv()
        to_chip(ALONG_X, n).wait_recv()
        to_chip(ALONG_Y, n).wait_recv()
        return n

    results = [extras[0], theirs.at[ACROSS]] if len(out_refs) > 1 else [extras[-1]]

    def put(n):
        return [pltpu.make_async_copy(b.at[n], r.at[:, cut(n)], osem.at[i, n]) for i, (r, b) in enumerate(zip(out_refs, results))]

    finish(slices, sum_of, ready, lambda n: begin(put(n)), extras, theirs.at[ACROSS])

    def end(n):
        finished(put(n))
        to_chip(ALONG_X, n).wait_send()
        to_chip(ALONG_Y, n).wait_send()

    loop(0, slices, end)


def reduce(name, number, take, terms, weights, extras, outs, finish, gflops, fillers=(), fill=(), fill_outs=()):
    d = extras[0].shape[1]
    slices = d // SLICE
    state = (slices, BLOCK, SLICE)
    both = 2 * BLOCK
    blocks = [(OWN, t.shape[0], both, t.shape[2]) if t.ndim == 3 else (OWN, both, t.shape[1]) for t in terms]
    nt = weights[0].shape[0] == d
    deep = sum(w.shape[nt] for w in weights)
    kept = (slices, SLICE, deep) if nt else (slices, deep, SLICE)
    dma = pltpu.SemaphoreType.DMA
    counts = (len(terms), len(weights), len(extras), len(fill), outs, len(fill_outs), len(terms), 1)
    low = lambda *shape: pltpu.VMEM(shape, LOW)
    return pl.pallas_call(
        functools.partial(_reduce, take, fillers, finish, counts),
        in_specs=[HBM] * sum(counts[:4]), out_specs=[HBM] * (outs + len(fill_outs)),
        out_shape=[jax.ShapeDtypeStruct((BLOCK, d), LOW)] * outs + [jax.ShapeDtypeStruct(s, LOW) for s in fill_outs],
        scratch_shapes=[*(low(*s) for s in blocks), low(*kept), low(*state), low(4, *state), low(OWN, *state), low(4, *state),
                        dma((OWN, len(terms), 2)), dma((len(weights), slices)), dma((len(extras), slices)), dma((outs, slices)), dma((4 * slices,)), dma((7 * slices,))],
        compiler_params=pltpu.CompilerParams(collective_id=number, has_side_effects=True, vmem_limit_bytes=ALL_VMEM),
        cost_estimate=work(gflops, 60), name=name,
    )(*terms, *weights, *extras, *fill)


def finish_norm(slices, sum_of, ready, put, extras, spare):
    (states,) = extras

    def one(i, squares):
        n = ready(i)
        h = (states[n].astype(jnp.float32) + sum_of(n)).astype(LOW)
        states[n] = h
        wide = h.astype(jnp.float32)
        return squares + jnp.sum(wide * wide, -1, keepdims=True)

    squares = lax.fori_loop(0, slices, one, jnp.zeros((BLOCK, 1), jnp.float32))
    scale = lax.rsqrt(squares / (slices * SLICE) + EPS)

    def two(n):
        spare[n] = (states[n].astype(jnp.float32) * scale).astype(LOW)
        put(n)

    loop(0, slices, two)


def finish_back(slices, sum_of, ready, put, extras, spare):
    states, rest = extras

    def one(i, so_far):
        n = ready(i)
        squares, across = so_far
        h, g = states[n].astype(jnp.float32), sum_of(n)
        return squares + jnp.sum(h * h, -1, keepdims=True), across + jnp.sum(h * g, -1, keepdims=True)

    zero = jnp.zeros((BLOCK, 1), jnp.float32)
    squares, across = lax.fori_loop(0, slices, one, (zero, zero))
    size = slices * SLICE
    scale = lax.rsqrt(squares / size + EPS)
    back = scale * scale * scale * (across / size)

    def two(n):
        by = sum_of(n) * scale - states[n].astype(jnp.float32) * back
        rest[n] = (rest[n].astype(jnp.float32) + by).astype(LOW)
        put(n)

    loop(0, slices, two)


def side_by_side(r):
    return [r[n] for n in range(r.shape[0])]


def heads_side_by_side(refs):
    return side_by_side(refs[0])


def as_they_are(refs):
    return [r[...] for r in refs]


def heads_and_two(refs):
    return side_by_side(refs[0]) + as_they_are(refs[1:])


WIDE = 512


def fill_by_hidden(part, refs, outs):
    dy_ref, wd_ref = refs
    (units, d), tokens = wd_ref.shape, dy_ref.shape[0]
    rows, wide = tokens // 2, units // 4

    def body(dy, w, out):
        out[...] = _nt(dy[...], w[...]).astype(LOW)

    pltpu.emit_pipeline(body, grid=(units // wide,), in_specs=[pl.BlockSpec((rows, d), lambda j: (part, 0)), pl.BlockSpec((wide, d), lambda j: (j, 0))],
                        out_specs=[pl.BlockSpec((rows, wide), lambda j: (part, j))])(dy_ref, wd_ref, outs[0])


def fill_by_wo(refs, outs):
    heads_ref, all_h_ref = refs[:2]
    g, tokens, _ = heads_ref.shape

    def body(heads, h, out):
        out[...] = _tn(jnp.concatenate(side_by_side(heads), axis=1), h[...]).astype(LOW)

    pltpu.emit_pipeline(body, grid=(all_h_ref.shape[1] // WIDE,), in_specs=[pl.BlockSpec((g, tokens, HEAD), lambda j: (0, 0, 0)),
                                                                          pl.BlockSpec((tokens, WIDE), lambda j: (0, j))],
                        out_specs=[pl.BlockSpec((g * HEAD, WIDE), lambda j: (0, j))])(heads_ref, all_h_ref, outs[0])


def fill_by_rest(refs, outs):
    a_ref, q_ref, k_ref, v_ref = refs[2:]
    g, tokens, _ = q_ref.shape
    one = pl.BlockSpec((tokens, HEAD), lambda j: (0, 0))
    narrow = pl.BlockSpec((WIDE, HEAD), lambda j: (j, 0))

    def body(a, q, k, v, by_q, by_k, by_v):
        t = _tn(a[...], jnp.concatenate(heads_and_two((q, k, v)), axis=1)).astype(LOW)
        by_q[...], by_k[...], by_v[...] = t[:, : g * HEAD], t[:, g * HEAD : (g + 1) * HEAD], t[:, (g + 1) * HEAD :]

    pltpu.emit_pipeline(body, grid=(a_ref.shape[1] // WIDE,),
                        in_specs=[pl.BlockSpec((tokens, WIDE), lambda j: (0, j)), pl.BlockSpec((g, tokens, HEAD), lambda j: (0, 0, 0)), one, one],
                        out_specs=[pl.BlockSpec((WIDE, g * HEAD), lambda j: (j, 0)), narrow, narrow])(a_ref, q_ref, k_ref, v_ref, *outs[1:])


def _by_heads(*refs):
    pieces, (wo_ref, heads_ref, all_ref, out_ref, delta_ref, states, wo, heads, outs, deltas, load_sem, store_sem, wo_sem) = refs[:-13], refs[-13:]
    me, (x, y, c), (dx, dy, _) = place()
    chips = (me, dx, dy, dx + 2 * (1 - 2 * y))
    per_chip = [pieces[n : n + 2] for n in (0, 2, 4)] + [pieces[6:]]
    weight = pltpu.make_async_copy(wo_ref, wo, wo_sem)
    here = [pl.ds(n * BLOCK, BLOCK) for n in range(2)]

    def copies(k, storing):
        at, pairs = 0, []
        rows = [rows_of(device) for device in (chips[k], chips[k] + 1 - 2 * c)]
        for piece in () if storing else per_chip[k]:
            pairs.append((piece, states.at[k, pl.ds(at, piece.shape[0])]))
            at += piece.shape[0]
        for mine, there in zip(here, rows):
            if storing:
                pairs += [(states.at[k, mine], all_ref.at[there]), (outs.at[k, :, mine], out_ref.at[:, there]), (deltas.at[k, :, mine], delta_ref.at[:, there])]
            else:
                pairs.append((heads_ref.at[:, there], heads.at[k, :, mine]))
        return [pltpu.make_async_copy(a, b, (store_sem if storing else load_sem).at[k, n]) for n, (a, b) in enumerate(pairs)]

    def each(act, k, storing):
        for copy in copies(k, storing):
            getattr(copy, act)()

    each("start", 0, False)
    weight.start()
    for k in range(1, GROUPS):
        each("start", k, False)
    weight.wait()

    def chip(k):
        for j in range(GROUPS):
            pl.when(k == j)(functools.partial(each, "wait", j, False))
        t = _nt(states[k], wo[...]).astype(LOW)
        for n in range(out_ref.shape[0]):
            part = t[:, n * HEAD : (n + 1) * HEAD]
            outs[k, n] = part
            deltas[k, n : n + 1, :] = (part.astype(jnp.float32) * heads[k, n].astype(jnp.float32)).T.sum(axis=0, keepdims=True)
        for j in range(GROUPS):
            pl.when(k == j)(functools.partial(each, "start", j, True))

    loop(0, GROUPS, chip)
    for k in range(GROUPS):
        each("wait", k, True)


def by_heads(pieces, wo, heads):
    g, tokens, _ = heads.shape
    d = wo.shape[1]
    dma = pltpu.SemaphoreType.DMA
    buffer = lambda *shape: pltpu.VMEM((GROUPS, *shape), LOW)
    return pl.pallas_call(
        _by_heads, in_specs=[pl.BlockSpec(memory_space=pl.ANY)] * len(pieces) + [HBM] * 2, out_specs=[HBM] * 3,
        out_shape=[jax.ShapeDtypeStruct((tokens, d), LOW), jax.ShapeDtypeStruct(heads.shape, LOW), jax.ShapeDtypeStruct((g, tokens), jnp.float32)],
        scratch_shapes=[buffer(CHIP, d), pltpu.VMEM(wo.shape, LOW), buffer(g, CHIP, HEAD), buffer(g, CHIP, HEAD),
                        pltpu.VMEM((GROUPS, g, CHIP), jnp.float32), dma((GROUPS, 6)), dma((GROUPS, 6)), dma],
        compiler_params=pltpu.CompilerParams(vmem_limit_bytes=36 * MIB), cost_estimate=work(9, 40), name="by_heads",
    )(*pieces, wo, heads)


def hop(t, distance):
    return lax.ppermute(t, "tp", [(n, n ^ distance) for n in range(8)])


def mm(eq, a, b):
    return jnp.einsum(eq, a, b, preferred_element_type=jnp.float32).astype(LOW)


def layer(x, dy, w):
    tokens, d = BLOCK * 8, x.shape[1]
    cos, sin = angles(tokens)
    a, q, k, v, all_dy, heads, lse, *across = project(x, dy, w["wq"], w["wk"], w["wv"], cos, sin, w["w_gate"], w["w_up"])
    units = w["w_down"].shape[0]
    h, b_own, by_hidden = reduce("add_heads", 2, heads_side_by_side, [heads], [w["wo"]], [x], 2, finish_norm, 60,
                                 [functools.partial(fill_by_hidden, part) for part in range(2)], [all_dy, w["w_down"]], [(tokens, units)])
    b, hidden, by_gate, by_up = hidden_units(b_own, by_hidden, w["w_gate"], w["w_up"])
    (by_h,) = reduce("by_states", 3, as_they_are, [by_gate, by_up], across, [h, dy], 1, finish_back, 80)
    on_x, on_y, on_chip = 4, 2, 1
    from_x, from_y, own2 = hop(by_h, on_x), hop(by_h, on_y), hop(by_h, on_chip)
    by_w = {"w_gate": mm("td,tu->du", b, by_gate), "w_up": mm("td,tu->du", b, by_up)}
    from_x, from_y, hidden, by_w = lax.optimization_barrier((from_x, from_y, hidden, by_w))
    far = [hop(from_y[:HALF], on_x), hop(from_x[HALF:], on_y)]
    x2, y2 = hop(from_x, on_chip), hop(from_y, on_chip)
    by_w["w_down"] = mm("tu,td->ud", hidden, all_dy)
    *far, by_w["w_down"] = lax.optimization_barrier((*far, by_w["w_down"]))
    pieces = [by_h, own2, from_x, x2, from_y, y2, *far, *(hop(t, on_chip) for t in far)]
    all_h, by_out, delta = by_heads(pieces, w["wo"], heads)
    by_q, by_k, by_v = attend_bwd(q, k, v, by_out, lse, delta, cos, sin)
    by_x, *rest = reduce("by_input", 4, heads_and_two, [by_q, by_k, by_v], [w["wq"], w["wk"], w["wv"]], [x, by_h], 1, finish_back, 60,
                         [fill_by_wo, fill_by_rest], [heads, all_h, a, by_q, by_k, by_v], [w[name].shape for name in ("wo", "wq", "wk", "wv")])
    by_w.update(zip(("wo", "wq", "wk", "wv"), rest))
    return by_x, by_w


def solution(mesh):
    def step(x, dy, *weights):
        by_x, by_w = layer(x[0], dy[0], dict(zip(NAMES, weights, strict=True)))
        return (by_x[None], *(by_w[name] for name in NAMES))

    states, by_columns, by_rows = P("dp", "tp", None), P(None, "tp"), P("tp", None)
    weights = (by_columns, by_columns, by_columns, by_rows, by_columns, by_columns, by_rows)
    own = tuple(P("dp", "tp") if spec == by_columns else P(("dp", "tp"), None) for spec in weights)
    return jax.shard_map(step, mesh=mesh, in_specs=(states, states, *weights), out_specs=(states, *own), check_vma=False)
```

```python
import functools

import jax
import jax.numpy as jnp
import numpy as np
from jax import lax
from jax.experimental import pallas as pl
from jax.experimental.pallas import tpu as pltpu
from jax.sharding import PartitionSpec as P

NEG = -1e30
HIDDEN = 2 * NEG
LOG2E = 1.4426950408889634
MIB = 2**20
VMEM, ALL_VMEM = 56 * MIB, 63 * MIB
STRIP = 512
KEYS = 512
QUERIES = QUERIES_BACK = 512
HEAD = 128
SUM_ROWS = 8
SCALE = HEAD**-0.5
E = SCALE * LOG2E


def _dot(a, b, ca, cb):
    return lax.dot_general(a, b, (((ca,), (cb,)), ((), ())), preferred_element_type=jnp.float32)


_nn, _nt, _tn = (functools.partial(_dot, ca=ca, cb=cb) for ca, cb in ((1, 0), (1, 1), (0, 0)))


def work(gflops, megabytes):
    return pl.CostEstimate(flops=gflops * 10**9, bytes_accessed=megabytes * 10**6, transcendentals=0)


def _seen(iq, bq):
    first = iq * bq
    return lax.div(first + 1, KEYS), lax.div(first + bq - 1 + KEYS, KEYS)


def _gap(cols, bq):
    return lax.rem(lax.broadcasted_iota(jnp.int32, (KEYS, cols), 1), bq) - lax.broadcasted_iota(jnp.int32, (KEYS, cols), 0)


def _row(ref):
    return jnp.concatenate([ref[n : n + 1, :] for n in range(ref.shape[0])], axis=1)


def _forward(q_ref, k_ref, v_ref, o_ref, lse_ref, top_s, mix_s, gap_s):
    g, bq, d = q_ref.shape
    cols = g * bq
    iq = pl.program_id(0)
    strips = range(0, cols, STRIP)
    gap_s[...] = _gap(cols, bq)
    top_s[...] = jnp.full_like(top_s, NEG)
    mix_s[...] = jnp.zeros_like(mix_s)
    ones = jnp.ones((SUM_ROWS, KEYS), k_ref.dtype)

    def block(j, masked):
        here = pl.ds(j * KEYS, KEYS)
        scores = [_nt(k_ref[here, :], q_ref[...].reshape(cols, d)[at : at + STRIP, :]) for at in strips]
        weights, keeps = [], []
        for at, s in zip(strips, scores):
            if masked:
                s = jnp.where(gap_s[:, at : at + STRIP] >= j * KEYS - iq * bq, s, HIDDEN)
            old = top_s[:, at : at + STRIP]
            top = jnp.maximum(old, s.max(axis=0, keepdims=True))
            top_s[:, at : at + STRIP] = top
            weights.append(jnp.exp2((s - top) * E).astype(k_ref.dtype))
            keeps.append(jnp.exp2((old - top) * E))
        for at, p, keep in zip(strips, weights, keeps):
            values = jnp.concatenate([v_ref[here, :].T, ones], axis=0)
            mix_s[:, at : at + STRIP] = mix_s[:, at : at + STRIP] * keep + _nn(values, p)

    whole, last = _seen(iq, bq)
    loop(0, whole, lambda j: block(j, False))
    loop(whole, last, lambda j: block(j, True))
    total = mix_s[d : d + 1, :]
    o_ref[...] = (mix_s[:d, :] * (1 / total)).T.reshape(g, bq, d).astype(o_ref.dtype)
    lse = top_s[...] * SCALE + jnp.log(total)
    for n in range(g):
        lse_ref[n : n + 1, :] = lse[:, n * bq : (n + 1) * bq]


def _cost(q, width):
    g, s, d = q.shape
    return pl.CostEstimate(flops=2 * g * s * s * width, transcendentals=g * s * s, bytes_accessed=4 * q.size * q.dtype.itemsize)


def _backward(q_ref, k_ref, v_ref, do_ref, lse_ref, delta_ref, cos_ref, sin_ref, dq_ref, dk_ref, dv_ref, dq_s, dk_s, dv_s, gap_s):
    g, bq, d = q_ref.shape
    cols, low = g * bq, q_ref.dtype
    iq = pl.program_id(0)
    strips = range(0, cols, STRIP)

    @pl.when(iq == 0)
    def _():
        gap_s[...] = _gap(cols, bq)
        dk_s[...] = jnp.zeros_like(dk_s)
        dv_s[...] = jnp.zeros_like(dv_s)

    dq_s[...] = jnp.zeros_like(dq_s)
    lses, deltas = _row(lse_ref) * LOG2E, _row(delta_ref)

    def block(j, masked):
        here = pl.ds(j * KEYS, KEYS)
        qs = [q_ref[...].reshape(cols, d)[at : at + STRIP, :] for at in strips]
        dos = [do_ref[...].reshape(cols, d)[at : at + STRIP, :] for at in strips]
        scores = [_nt(k_ref[here, :], x) for x in qs]
        dps = [_nt(v_ref[here, :], x) for x in dos]
        for n, at in enumerate(strips):
            p = jnp.exp2(scores[n] * E - lses[:, at : at + STRIP])
            if masked:
                p = jnp.where(gap_s[:, at : at + STRIP] >= j * KEYS - iq * bq, p, 0.0)
            ds = (p * (dps[n] - deltas[:, at : at + STRIP])).astype(low)
            dv_s[here, :] += _nn(p.astype(low), dos[n])
            dk_s[here, :] += _nn(ds, qs[n])
            dq_s[:, at : at + STRIP] += _nn(k_ref[here, :].T, ds)

    whole, last = _seen(iq, bq)
    loop(0, whole, lambda j: block(j, False))
    loop(whole, last, lambda j: block(j, True))
    here = pl.ds(iq * bq, bq)
    by_q = (dq_s[...] * SCALE).T
    cos, sin = cos_ref[here, :], sin_ref[here, :]
    for n in range(g):
        dq_ref[n] = turn(by_q[n * bq : (n + 1) * bq, :], cos, -sin)

    @pl.when(iq == pl.num_programs(0) - 1)
    def _():
        dk_ref[...] = turn(dk_s[...] * SCALE, cos_ref[...], -sin_ref[...])
        dv_ref[...] = dv_s[...].astype(dv_ref.dtype)


def attend_bwd(q, k, v, d_out, lse, delta, cos, sin):
    g, s, d = q.shape
    bq = QUERIES_BACK
    queries = pl.BlockSpec((g, bq, d), lambda i: (0, i, 0))
    keys = pl.BlockSpec((s, d), lambda i: (0, 0))
    table = pl.BlockSpec(cos.shape, lambda i: (0, 0))
    stats = pl.BlockSpec((g, bq), lambda i: (0, i))
    return pl.pallas_call(
        _backward, grid=(s // bq,), in_specs=[queries, keys, keys, queries, stats, stats, table, table], out_specs=[queries, keys, keys],
        scratch_shapes=[pltpu.VMEM((d, g * bq), jnp.float32), pltpu.VMEM((s, d), jnp.float32), pltpu.VMEM((s, d), jnp.float32),
                        pltpu.VMEM((KEYS, g * bq), jnp.int32)],
        out_shape=[jax.ShapeDtypeStruct(t.shape, t.dtype) for t in (q, k, v)],
        compiler_params=pltpu.CompilerParams(dimension_semantics=("arbitrary",), vmem_limit_bytes=VMEM), cost_estimate=_cost(q, 5 * d), name="attend_bwd",
    )(q, k, v, d_out, lse, delta, cos, sin)


THETA = 10000
NAMES = ("wq", "wk", "wv", "wo", "w_gate", "w_up", "w_down")
EPS = 1e-6
LOW = jnp.bfloat16
BLOCK = 256
SLICE = 512
HBM = pl.BlockSpec(memory_space=pltpu.HBM)


def normed(h):
    wide = h.astype(jnp.float32)
    scale = lax.rsqrt(jnp.mean(wide**2, -1, keepdims=True) + EPS)
    return (wide * scale).astype(jnp.bfloat16)


def place():
    me = lax.axis_index("tp")
    x, y, c = lax.div(me, 4), lax.rem(lax.div(me, 2), 2), lax.rem(me, 2)
    return me, (x, y, c), (me + 4 * (1 - 2 * x), me + 2 * (1 - 2 * y), me + 1 - 2 * c)


def greet(neighbours):
    barrier = pltpu.get_barrier_semaphore()
    for device in neighbours:
        pl.semaphore_signal(barrier, inc=1, device_id={"tp": device}, device_id_type=pl.DeviceIdType.MESH)
    pl.semaphore_wait(barrier, len(neighbours))


def send(src, dst, sems, n, device):
    return pltpu.make_async_remote_copy(src_ref=src, dst_ref=dst, send_sem=sems[0].at[n], recv_sem=sems[1].at[n], device_id={"tp": device},
                                        device_id_type=pl.DeviceIdType.MESH)


def rows_of(device, half=None):
    if half is None:
        return pl.ds(pl.multiple_of(device * BLOCK, BLOCK), BLOCK)
    return pl.ds(pl.multiple_of(device * BLOCK + half * (BLOCK // 2), BLOCK // 2), BLOCK // 2)


def loop(start, end, f):
    def step(i, _):
        f(i)

    lax.fori_loop(start, end, step, None)


HALF = BLOCK // 2
CHIP = 2 * BLOCK
GROUPS = 4


WAYS, FINE_WAYS = ([[[int(n) for n in way.split("-")] for way in ways.split()] for ways in groups] for groups in (
    ("0", "3-5-8 1-6-7 7 8", "2-9 4-10 9 10", "5-11 6-12 11 12"),
    ("0", "3-5-7-10 1-6-8-9 9 10", "2-11 4-12 11 12", "5-13 6-14 13 14", "7-15 8-16 15 16")))


class Gather:
    def __init__(self, own_ref, all_ref, sems, local, store=None, kept=None):
        self.own_ref, self.all_ref, self.store, self.local, self.kept = own_ref, all_ref, store, local, kept
        me, (x, y, c), (dx, dy, dc) = place()
        self.at, self.near = (x, y, c), (dx, dy, dc)
        parts = range(2)
        if store is None:
            size = HALF // 2
            rows = lambda device, at, size: all_ref.at[pl.ds(pl.multiple_of(device * BLOCK + at, HALF // 2), size)]
            half = lambda device, n: rows(device, n * HALF, HALF)
            fine = lambda device, n: [rows(device, n * HALF + r * size, size) for r in parts]
            self.own, own, self.ways = own_ref, all_ref.at[rows_of(me)], FINE_WAYS
            mine = [own_ref.at[pl.ds(n * HALF, HALF)] for n in parts]
            x1, x2, y1, y2 = half(me, 1), half(me, 0), half(me, 0), half(me, 1)
            came = [half(dx, 1), half(dy, 0), half(dx, 0), half(dy, 1)]
            onward = [(t, t, to) for pair in zip(fine(dy, 0), fine(dx, 1)) for t, to in zip(pair, (dx, dy))]
            came += [t for pair in zip(*(fine(dx + 2 * (1 - 2 * y), n) for n in parts)) for t in pair]
        else:
            slot = lambda group, i, n=1: store.at[pl.ds(pl.multiple_of(group * CHIP + i * HALF, HALF), n * HALF)]
            own = self.own = slot(0, 2 * c, 2)
            self.ways = WAYS
            mine = (slot(0, 2 * c), slot(0, 2 * c + 1))
            came = x1, y1, x2, y2, d0, d1 = [slot(g, i) for g, i in ((1, c), (1, 2 + c), (2, c), (2, 2 + c), (3, 2 * c), (3, 2 * c + 1))]
            onward = [(y1, d0, dx), (x1, d1, dy)]
        steps = [(self.own, own, dc), (mine[1], x1, dx), (mine[0], x2, dx), (mine[0], y1, dy), (mine[1], y2, dy), *onward, *((t, t, dc) for t in came)]
        self.copies = [send(a, b, sems, n, to) for n, (a, b, to) in enumerate(steps)]

    def begin(self, change=None):
        load = pltpu.make_async_copy(self.own_ref, self.own, self.local.at[0])
        load.start()
        load.wait()
        if change is not None:
            rows = 32

            def some(n):
                here = pl.ds(pl.multiple_of(2 * HALF * self.at[2] + n * rows, rows), rows)
                self.store[here, :] = change(self.store[here, :])

            loop(0, BLOCK // rows, some)
        greet(self.near)
        self.start()

    def start(self):
        for n in (1, 3, 2, 4, 0):
            self.copies[n].start()

    def arrive(self, group):
        for k in range(GROUPS):
            pl.when(group == k)(functools.partial(self.take, k))
        for i in range(GROUPS):
            self.keep(group, i).start()

    def take(self, group):
        for n, *onward in self.ways[group]:
            self.copies[n].wait_recv()
            for m in onward:
                self.copies[m].start()

    def rows(self, group, i):
        x, y, c = self.at
        mixed = (group == 1) | (group == 2)
        turn_x = jnp.where(mixed, 1 if i < 2 else 0, lax.div(group, 3))
        turn_y = jnp.where(mixed, 0 if i < 2 else 1, lax.div(group, 3))
        core = jnp.where(mixed, i % 2, i // 2)
        half = jnp.where(mixed, 2 - group if i < 2 else group - 1, i % 2)
        device = (x + turn_x * (1 - 2 * x)) * 4 + (y + turn_y * (1 - 2 * y)) * 2 + core
        return device * 2 + half

    def keep(self, group, i):
        here = pl.ds(pl.multiple_of(group * CHIP + i * HALF, HALF), HALF)
        there = pl.ds(pl.multiple_of(self.rows(group, i) * HALF, HALF), HALF)
        return pltpu.make_async_copy(self.store.at[here], self.all_ref.at[there], self.kept.at[group, i])

    def states(self, group):
        return self.store[pl.ds(pl.multiple_of(group * CHIP, CHIP), CHIP), :]

    def end(self):
        def some(group):
            for i in range(GROUPS):
                self.keep(group, i).wait()

        if self.store is not None:
            loop(0, GROUPS, some)
        for copy in self.copies:
            copy.wait_send()


def gather_scratch(tokens, d):
    dma = pltpu.SemaphoreType.DMA
    return [pltpu.VMEM((tokens, d), LOW), dma((1,)), dma((GROUPS, GROUPS)), dma((17,)), dma((17,))]


def turn(t, cos, sin):
    half = HEAD // 2
    other = jnp.concatenate([t[:, half:], t[:, :half]], axis=1)
    return (t * jnp.concatenate([cos, cos], axis=1) + other * jnp.concatenate([-sin, sin], axis=1)).astype(LOW)


def angles(tokens):
    half = HEAD // 2
    angle = np.arange(tokens, dtype=np.float32)[:, None] * THETA ** (-np.arange(half, dtype=np.float32) / half)
    return jnp.asarray(np.cos(angle), jnp.float32), jnp.asarray(np.sin(angle), jnp.float32)


def _project(own_ref, dy_ref, wq_ref, wk_ref, wv_ref, cos_ref, sin_ref, wg_ref, wu_ref, all_ref, q_ref, k_ref, v_ref, all_dy_ref, o_ref, lse_ref,
             wg_across_ref, wu_across_ref, store, local, kept, ssem, rsem, wq, wk, wv, wsem, block, dy_ssem, dy_rsem, *scratch):
    gather = Gather(own_ref, all_ref, (ssem, rsem), local, store, kept)
    loads = [pltpu.make_async_copy(a, b, wsem.at[n]) for n, (a, b) in enumerate(((wq_ref, wq), (wk_ref, wk), (wv_ref, wv)))]
    for load in loads:
        load.start()
    gather.begin(normed)
    dy = Gather(dy_ref, all_dy_ref, (dy_ssem, dy_rsem), local)
    keep = pltpu.make_async_copy(dy_ref, block, local.at[0])
    keep.start()
    for load in loads:
        load.wait()
    keep.wait()
    keep = pltpu.make_async_copy(block, all_dy_ref.at[rows_of(lax.axis_index("tp"))], local.at[0])
    keep.start()

    def group(k):
        gather.arrive(k)
        pl.when(k == 1)(dy.start)

        def body(*refs):
            coses, sins, qs, ks, vs = (refs[n * GROUPS : (n + 1) * GROUPS] for n in range(5))
            t = gather.states(k)
            by_q, by_k, by_v = (_nn(t, w[...]).astype(LOW).astype(jnp.float32) for w in (wq, wk, wv))
            for i in range(GROUPS):
                rows = slice(i * HALF, (i + 1) * HALF)
                cos, sin = coses[i][...], sins[i][...]
                for n in range(q_ref.shape[0]):
                    qs[i][n] = turn(by_q[rows, n * HEAD : (n + 1) * HEAD], cos, sin)
                ks[i][...] = turn(by_k[rows], cos, sin)
                vs[i][...] = by_v[rows].astype(LOW)

        heads, one, table = [], [], []
        for i in range(GROUPS):
            at = gather.rows(k, i)
            heads.append(pl.BlockSpec((q_ref.shape[0], HALF, HEAD), lambda j, at=at: (0, at, 0)))
            one.append(pl.BlockSpec((HALF, HEAD), lambda j, at=at: (at, 0)))
            table.append(pl.BlockSpec((HALF, cos_ref.shape[1]), lambda j, at=at: (at, 0)))
        pltpu.emit_pipeline(body, grid=(1,), in_specs=[*table, *table], out_specs=[*heads, *one, *one])(
            *(ref for ref in (cos_ref, sin_ref, q_ref, k_ref, v_ref) for _ in range(GROUPS)))

    loop(0, GROUPS, group)
    g, tokens, d = q_ref.shape
    queries = pl.BlockSpec((g, QUERIES, d), lambda i: (0, i, 0))
    keys = pl.BlockSpec((tokens, d), lambda i: (0, 0))
    pltpu.emit_pipeline(lambda *refs: _forward(*refs, *scratch), grid=(tokens // QUERIES,), in_specs=[queries, keys, keys],
                        out_specs=[queries, pl.BlockSpec((g, QUERIES), lambda i: (0, i))])(q_ref, k_ref, v_ref, o_ref, lse_ref)
    dy.take(0)
    dy.take(1)

    def lay(*refs):
        for a, b in zip(refs[:2], refs[2:]):
            b[...] = a[...].T

    d, units = wg_ref.shape
    tall, flat = pl.BlockSpec((BLOCK, units), lambda i: (i, 0)), pl.BlockSpec((units, BLOCK), lambda i: (0, i))
    pltpu.emit_pipeline(lay, grid=(d // BLOCK,), in_specs=[tall] * 2, out_specs=[flat] * 2)(wg_ref, wu_ref, wg_across_ref, wu_across_ref)
    for k in range(2, len(FINE_WAYS)):
        dy.take(k)
    keep.wait()
    dy.end()
    gather.end()


def project(own, dy, wq, wk, wv, cos, sin, w_gate, w_up):
    d, tokens = own.shape[1], cos.shape[0]
    one, states = jax.ShapeDtypeStruct((tokens, HEAD), LOW), jax.ShapeDtypeStruct((tokens, d), LOW)
    g = wq.shape[1] // HEAD
    heads = jax.ShapeDtypeStruct((g, tokens, HEAD), LOW)
    block, *_, ssem, rsem = gather_scratch(BLOCK, d)
    cols = g * QUERIES
    across = jax.ShapeDtypeStruct(w_gate.shape[::-1], LOW)
    return pl.pallas_call(
        _project, in_specs=[HBM] * 9, out_specs=[HBM] * 9,
        out_shape=[states, heads, one, one, states, heads, jax.ShapeDtypeStruct((g, tokens), jnp.float32), across, across],
        scratch_shapes=[*gather_scratch(tokens, d), *(pltpu.VMEM(w.shape, LOW) for w in (wq, wk, wv)), pltpu.SemaphoreType.DMA((3,)), block, ssem, rsem,
                        pltpu.VMEM((1, cols), jnp.float32), pltpu.VMEM((HEAD + SUM_ROWS, cols), jnp.float32), pltpu.VMEM((KEYS, cols), jnp.int32)],
        compiler_params=pltpu.CompilerParams(collective_id=0, has_side_effects=True, vmem_limit_bytes=ALL_VMEM), cost_estimate=work(70, 60), name="project",
    )(own, dy, wq, wk, wv, cos, sin, w_gate, w_up)


NARROW = 256


def _hidden(own_ref, by_hidden_ref, wg_ref, wu_ref, all_ref, hidden_ref, by_gate_ref, by_up_ref, store, local, kept, ssem, rsem, wg, wu, wsem):
    gather = Gather(own_ref, all_ref, (ssem, rsem), local, store, kept)
    tiles = wg.shape[0]

    def weights(n):
        cut = pl.ds(pl.multiple_of(n * NARROW, NARROW), NARROW)
        return [pltpu.make_async_copy(a.at[:, cut], b.at[n], wsem.at[i, n]) for i, (a, b) in enumerate(((wg_ref, wg), (wu_ref, wu)))]

    gather.begin()
    loop(0, tiles, lambda n: [copy.start() for copy in weights(n)] and None)

    def group(k):
        gather.arrive(k)

        def body(*refs):
            bys, hiddens, by_gates, by_ups = (refs[n * GROUPS : (n + 1) * GROUPS] for n in range(4))
            j = pl.program_id(0)

            @pl.when(k == 0)
            def _():
                for copy in weights(j):
                    copy.wait()

            t = gather.states(k)
            gate, up = _nn(t, wg[j]), _nn(t, wu[j])
            for i in range(GROUPS):
                rows = slice(i * HALF, (i + 1) * HALF)
                g, u, by = gate[rows], up[rows], bys[i][...].astype(jnp.float32)
                s = jax.nn.sigmoid(g)
                silu = g * s
                hiddens[i][...] = (silu * u).astype(LOW)
                by_ups[i][...] = (by * silu).astype(LOW)
                by_gates[i][...] = (by * u * (s + silu * (1 - s))).astype(LOW)

        piece = [pl.BlockSpec((HALF, NARROW), lambda j, at=gather.rows(k, i): (at, j)) for i in range(GROUPS)]
        pltpu.emit_pipeline(body, grid=(tiles,), in_specs=piece, out_specs=piece * 3)(
            *(ref for ref in (by_hidden_ref, hidden_ref, by_gate_ref, by_up_ref) for _ in range(GROUPS)))

    loop(0, GROUPS, group)
    gather.end()


def hidden_units(own, by_hidden, w_gate, w_up):
    tokens, units = by_hidden.shape
    d = own.shape[1]
    part = jax.ShapeDtypeStruct((tokens, units), LOW)
    kept = pltpu.VMEM((units // NARROW, d, NARROW), LOW)
    return pl.pallas_call(
        _hidden, in_specs=[HBM] * 4, out_specs=[HBM] * 4, out_shape=[jax.ShapeDtypeStruct((tokens, d), LOW), part, part, part],
        scratch_shapes=[*gather_scratch(tokens, d), kept, kept, pltpu.SemaphoreType.DMA((2, units // NARROW))],
        compiler_params=pltpu.CompilerParams(collective_id=1, has_side_effects=True, vmem_limit_bytes=ALL_VMEM),
        cost_estimate=work(90, 200), name="hidden_units",
    )(own, by_hidden, w_gate, w_up)


ACROSS, ALONG_X, ALONG_Y, OWN = range(4)
SLICES = 8


def _unit(u):
    part, pair, odd = lax.div(u, SLICES), lax.div(lax.rem(u, SLICES), 2), lax.rem(u, 2)
    chip = jnp.where(part == 0, ACROSS, jnp.where(part == 3, OWN, 1 + odd))
    late = jnp.where(part == 2, 1 - odd, odd)
    return chip, late * (SLICES // 2) + pair


def _reduce(take, fillers, finish, counts, *refs):
    groups = []
    for count in counts:
        groups.append(refs[:count])
        refs = refs[count:]
    a_refs, w_refs, extra_refs, fill_refs, out_refs, fill_outs, a_bufs, (w_buf,) = groups
    mine, theirs, came, passed, asem, wsem, esem, osem, ssem, rsem = refs
    slices = mine.shape[0]
    half = slices // 2
    me, (x, y, c), (dx, dy, dc) = place()
    nt = w_refs[0].shape[0] == slices * SLICE
    cut = lambda n: pl.ds(pl.multiple_of(n * SLICE, SLICE), SLICE)

    def weights(n):
        at, copies = 0, []
        for i, ref in enumerate(w_refs):
            deep = pl.ds(at, ref.shape[nt])
            at += ref.shape[nt]
            pair = (ref.at[cut(n)], w_buf.at[n, :, deep]) if nt else (ref.at[:, cut(n)], w_buf.at[n, deep])
            copies.append(pltpu.make_async_copy(*pair, wsem.at[i, n]))
        return copies

    chips = (dx + 2 * (1 - 2 * y), dx, dy, me)

    def load(m):
        copies = []
        for s, device in enumerate((chips[m], chips[m] + 1 - 2 * c)):
            for i, (ref, buf) in enumerate(zip(a_refs, a_bufs)):
                at = pl.ds(s * BLOCK, BLOCK)
                copies.append(pltpu.make_async_copy(ref.at[:, rows_of(device)], buf.at[m % OWN, :, at], asem.at[m % OWN, i, s]) if len(ref.shape) == 3 else
                              pltpu.make_async_copy(ref.at[rows_of(device)], buf.at[m % OWN, at], asem.at[m % OWN, i, s]))
        return copies

    def begin(copies):
        for copy in copies:
            copy.start()

    def finished(copies):
        for copy in copies:
            copy.wait()

    over = functools.partial(pltpu.make_async_remote_copy, device_id_type=pl.DeviceIdType.MESH)

    def to_core(m, n):
        return over(mine.at[n], theirs.at[m, n], ssem.at[n], rsem.at[m * slices + n], device_id={"tp": dc})

    def to_chip(m, n):
        along_x = (m == ALONG_X) | ((m == ACROSS) & (n < half))
        return over(passed.at[m, n], came.at[m, n], ssem.at[(m + 1) * slices + n], rsem.at[(m + 4) * slices + n], device_id={"tp": jnp.where(along_x, dx, dy)})

    def order(i):
        return lax.rem(i, 2) * half + lax.div(i, 2)

    begin(load(ACROSS))
    loop(0, slices, lambda i: begin(weights(order(i))))
    begin(load(ALONG_X))
    begin(load(ALONG_Y))
    greet((dx, dy, dc))

    def add(m, n, *terms):
        passed[m, n] = sum((t.astype(jnp.float32) for t in terms), passed[m, n].astype(jnp.float32)).astype(LOW)

    def join(u):
        m, n = _unit(u)
        to_core(m, n).wait_recv()
        far = u >= 2 * slices

        @pl.when(far)
        def _():
            to_chip(ACROSS, n).wait_recv()
            add(m, n, theirs[m, n], came[ACROSS, n])

        @pl.when(u < 2 * slices)
        def _():
            add(m, n, theirs[m, n])

        to_chip(m, n).start()

    first = {ACROSS: [lambda: finished(load(ACROSS))], ALONG_X: [lambda: finished(load(ALONG_X) + load(ALONG_Y)), lambda: begin(load(OWN))],
             ALONG_Y: [functools.partial(f, fill_refs, fill_outs) for f in fillers[:1]], OWN: [lambda: finished(load(OWN))]}

    def unit(u):
        m, n = _unit(u)
        for at, acts in first.items():

            @pl.when(u == at * slices)
            def _(acts=acts):
                for act in acts:
                    act()

        @pl.when(u < slices)
        def _():
            finished(weights(n))

        pl.when(u >= slices)(lambda: to_core(m, n).wait_send())
        t = jnp.concatenate(take([b.at[lax.rem(m, OWN)] for b in a_bufs]), axis=1)
        acc = (_nt if nt else _nn)(t, w_buf[n]).astype(LOW)
        passed[m, n] = acc[:BLOCK]
        mine[n] = acc[BLOCK:]
        to_core(m, n).start()
        pl.when((u > 0) & (u <= OWN * slices))(lambda: join(u - 1))

    loop(0, 4 * slices, unit)
    for fill in fillers[1:]:
        fill(fill_refs, fill_outs)

    def gone(n):
        to_core(OWN, n).wait_send()
        to_chip(ACROSS, n).wait_send()

    loop(0, slices, gone)
    extras = [passed.at[ACROSS], mine][: len(extra_refs)]
    slice_copies = lambda pairs, sem, n: [pltpu.make_async_copy(r.at[:, cut(n)], b.at[n], sem.at[i, n]) for i, (r, b) in enumerate(pairs)]
    loads = list(zip(extra_refs, extras))
    loop(0, slices, lambda n: begin(slice_copies(loads, esem, n)))
    loop(0, slices, lambda n: finished(slice_copies(loads, esem, n)))
    def sum_of(n):
        return sum(t.astype(jnp.float32) for t in (passed[OWN, n], theirs[OWN, n], came[ALONG_X, n], came[ALONG_Y, n]))

    def ready(i):
        n = order(i)
        to_core(OWN, n).wait_recv()
        to_chip(ALONG_X, n).wait_recv()
        to_chip(ALONG_Y, n).wait_recv()
        return n

    results = [extras[0], theirs.at[ACROSS]] if len(out_refs) > 1 else [extras[-1]]

    def put(n):
        return [pltpu.make_async_copy(b.at[n], r.at[:, cut(n)], osem.at[i, n]) for i, (r, b) in enumerate(zip(out_refs, results))]

    finish(slices, sum_of, ready, lambda n: begin(put(n)), extras, theirs.at[ACROSS])

    def end(n):
        finished(put(n))
        to_chip(ALONG_X, n).wait_send()
        to_chip(ALONG_Y, n).wait_send()

    loop(0, slices, end)


def reduce(name, number, take, terms, weights, extras, outs, finish, gflops, fillers=(), fill=(), fill_outs=()):
    d = extras[0].shape[1]
    slices = d // SLICE
    state = (slices, BLOCK, SLICE)
    both = 2 * BLOCK
    blocks = [(OWN, t.shape[0], both, t.shape[2]) if t.ndim == 3 else (OWN, both, t.shape[1]) for t in terms]
    nt = weights[0].shape[0] == d
    deep = sum(w.shape[nt] for w in weights)
    kept = (slices, SLICE, deep) if nt else (slices, deep, SLICE)
    dma = pltpu.SemaphoreType.DMA
    counts = (len(terms), len(weights), len(extras), len(fill), outs, len(fill_outs), len(terms), 1)
    low = lambda *shape: pltpu.VMEM(shape, LOW)
    return pl.pallas_call(
        functools.partial(_reduce, take, fillers, finish, counts),
        in_specs=[HBM] * sum(counts[:4]), out_specs=[HBM] * (outs + len(fill_outs)),
        out_shape=[jax.ShapeDtypeStruct((BLOCK, d), LOW)] * outs + [jax.ShapeDtypeStruct(s, LOW) for s in fill_outs],
        scratch_shapes=[*(low(*s) for s in blocks), low(*kept), low(*state), low(4, *state), low(OWN, *state), low(4, *state),
                        dma((OWN, len(terms), 2)), dma((len(weights), slices)), dma((len(extras), slices)), dma((outs, slices)), dma((4 * slices,)), dma((7 * slices,))],
        compiler_params=pltpu.CompilerParams(collective_id=number, has_side_effects=True, vmem_limit_bytes=ALL_VMEM),
        cost_estimate=work(gflops, 60), name=name,
    )(*terms, *weights, *extras, *fill)


def finish_norm(slices, sum_of, ready, put, extras, spare):
    (states,) = extras

    def one(i, squares):
        n = ready(i)
        h = (states[n].astype(jnp.float32) + sum_of(n)).astype(LOW)
        states[n] = h
        wide = h.astype(jnp.float32)
        return squares + jnp.sum(wide * wide, -1, keepdims=True)

    squares = lax.fori_loop(0, slices, one, jnp.zeros((BLOCK, 1), jnp.float32))
    scale = lax.rsqrt(squares / (slices * SLICE) + EPS)

    def two(n):
        spare[n] = (states[n].astype(jnp.float32) * scale).astype(LOW)
        put(n)

    loop(0, slices, two)


def finish_back(slices, sum_of, ready, put, extras, spare):
    states, rest = extras

    def one(i, so_far):
        n = ready(i)
        squares, across = so_far
        h, g = states[n].astype(jnp.float32), sum_of(n)
        return squares + jnp.sum(h * h, -1, keepdims=True), across + jnp.sum(h * g, -1, keepdims=True)

    zero = jnp.zeros((BLOCK, 1), jnp.float32)
    squares, across = lax.fori_loop(0, slices, one, (zero, zero))
    size = slices * SLICE
    scale = lax.rsqrt(squares / size + EPS)
    back = scale * scale * scale * (across / size)

    def two(n):
        by = sum_of(n) * scale - states[n].astype(jnp.float32) * back
        rest[n] = (rest[n].astype(jnp.float32) + by).astype(LOW)
        put(n)

    loop(0, slices, two)


def side_by_side(r):
    return [r[n] for n in range(r.shape[0])]


def heads_side_by_side(refs):
    return side_by_side(refs[0])


def as_they_are(refs):
    return [r[...] for r in refs]


def heads_and_two(refs):
    return side_by_side(refs[0]) + as_they_are(refs[1:])


WIDE = 512


def fill_by_hidden(part, refs, outs):
    dy_ref, wd_ref = refs
    (units, d), tokens = wd_ref.shape, dy_ref.shape[0]
    rows, wide = tokens // 2, units // 4

    def body(dy, w, out):
        out[...] = _nt(dy[...], w[...]).astype(LOW)

    pltpu.emit_pipeline(body, grid=(units // wide,), in_specs=[pl.BlockSpec((rows, d), lambda j: (part, 0)), pl.BlockSpec((wide, d), lambda j: (j, 0))],
                        out_specs=[pl.BlockSpec((rows, wide), lambda j: (part, j))])(dy_ref, wd_ref, outs[0])


def fill_by_wo(refs, outs):
    heads_ref, all_h_ref = refs[:2]
    g, tokens, _ = heads_ref.shape

    def body(heads, h, out):
        out[...] = _tn(jnp.concatenate(side_by_side(heads), axis=1), h[...]).astype(LOW)

    pltpu.emit_pipeline(body, grid=(all_h_ref.shape[1] // WIDE,), in_specs=[pl.BlockSpec((g, tokens, HEAD), lambda j: (0, 0, 0)),
                                                                          pl.BlockSpec((tokens, WIDE), lambda j: (0, j))],
                        out_specs=[pl.BlockSpec((g * HEAD, WIDE), lambda j: (0, j))])(heads_ref, all_h_ref, outs[0])


def fill_by_rest(refs, outs):
    a_ref, q_ref, k_ref, v_ref = refs[2:]
    g, tokens, _ = q_ref.shape
    one = pl.BlockSpec((tokens, HEAD), lambda j: (0, 0))
    narrow = pl.BlockSpec((WIDE, HEAD), lambda j: (j, 0))

    def body(a, q, k, v, by_q, by_k, by_v):
        t = _tn(a[...], jnp.concatenate(heads_and_two((q, k, v)), axis=1)).astype(LOW)
        by_q[...], by_k[...], by_v[...] = t[:, : g * HEAD], t[:, g * HEAD : (g + 1) * HEAD], t[:, (g + 1) * HEAD :]

    pltpu.emit_pipeline(body, grid=(a_ref.shape[1] // WIDE,),
                        in_specs=[pl.BlockSpec((tokens, WIDE), lambda j: (0, j)), pl.BlockSpec((g, tokens, HEAD), lambda j: (0, 0, 0)), one, one],
                        out_specs=[pl.BlockSpec((WIDE, g * HEAD), lambda j: (j, 0)), narrow, narrow])(a_ref, q_ref, k_ref, v_ref, *outs[1:])


def _by_heads(*refs):
    pieces, (wo_ref, heads_ref, all_ref, out_ref, delta_ref, states, wo, heads, outs, deltas, load_sem, store_sem, wo_sem) = refs[:-13], refs[-13:]
    me, (x, y, c), (dx, dy, _) = place()
    chips = (me, dx, dy, dx + 2 * (1 - 2 * y))
    per_chip = [pieces[n : n + 2] for n in (0, 2, 4)] + [pieces[6:]]
    weight = pltpu.make_async_copy(wo_ref, wo, wo_sem)
    here = [pl.ds(n * BLOCK, BLOCK) for n in range(2)]

    def copies(k, storing):
        at, pairs = 0, []
        rows = [rows_of(device) for device in (chips[k], chips[k] + 1 - 2 * c)]
        for piece in () if storing else per_chip[k]:
            pairs.append((piece, states.at[k, pl.ds(at, piece.shape[0])]))
            at += piece.shape[0]
        for mine, there in zip(here, rows):
            if storing:
                pairs += [(states.at[k, mine], all_ref.at[there]), (outs.at[k, :, mine], out_ref.at[:, there]), (deltas.at[k, :, mine], delta_ref.at[:, there])]
            else:
                pairs.append((heads_ref.at[:, there], heads.at[k, :, mine]))
        return [pltpu.make_async_copy(a, b, (store_sem if storing else load_sem).at[k, n]) for n, (a, b) in enumerate(pairs)]

    def each(act, k, storing):
        for copy in copies(k, storing):
            getattr(copy, act)()

    each("start", 0, False)
    weight.start()
    for k in range(1, GROUPS):
        each("start", k, False)
    weight.wait()

    def chip(k):
        for j in range(GROUPS):
            pl.when(k == j)(functools.partial(each, "wait", j, False))
        t = _nt(states[k], wo[...]).astype(LOW)
        for n in range(out_ref.shape[0]):
            part = t[:, n * HEAD : (n + 1) * HEAD]
            outs[k, n] = part
            deltas[k, n : n + 1, :] = (part.astype(jnp.float32) * heads[k, n].astype(jnp.float32)).T.sum(axis=0, keepdims=True)
        for j in range(GROUPS):
            pl.when(k == j)(functools.partial(each, "start", j, True))

    loop(0, GROUPS, chip)
    for k in range(GROUPS):
        each("wait", k, True)


def by_heads(pieces, wo, heads):
    g, tokens, _ = heads.shape
    d = wo.shape[1]
    dma = pltpu.SemaphoreType.DMA
    buffer = lambda *shape: pltpu.VMEM((GROUPS, *shape), LOW)
    return pl.pallas_call(
        _by_heads, in_specs=[pl.BlockSpec(memory_space=pl.ANY)] * len(pieces) + [HBM] * 2, out_specs=[HBM] * 3,
        out_shape=[jax.ShapeDtypeStruct((tokens, d), LOW), jax.ShapeDtypeStruct(heads.shape, LOW), jax.ShapeDtypeStruct((g, tokens), jnp.float32)],
        scratch_shapes=[buffer(CHIP, d), pltpu.VMEM(wo.shape, LOW), buffer(g, CHIP, HEAD), buffer(g, CHIP, HEAD),
                        pltpu.VMEM((GROUPS, g, CHIP), jnp.float32), dma((GROUPS, 6)), dma((GROUPS, 6)), dma],
        compiler_params=pltpu.CompilerParams(vmem_limit_bytes=36 * MIB), cost_estimate=work(9, 40), name="by_heads",
    )(*pieces, wo, heads)


def hop(t, distance):
    return lax.ppermute(t, "tp", [(n, n ^ distance) for n in range(8)])


def mm(eq, a, b):
    return jnp.einsum(eq, a, b, preferred_element_type=jnp.float32).astype(LOW)


def layer(x, dy, w):
    tokens, d = BLOCK * 8, x.shape[1]
    cos, sin = angles(tokens)
    a, q, k, v, all_dy, heads, lse, *across = project(x, dy, w["wq"], w["wk"], w["wv"], cos, sin, w["w_gate"], w["w_up"])
    units = w["w_down"].shape[0]
    h, b_own, by_hidden = reduce("add_heads", 2, heads_side_by_side, [heads], [w["wo"]], [x], 2, finish_norm, 60,
                                 [functools.partial(fill_by_hidden, part) for part in range(2)], [all_dy, w["w_down"]], [(tokens, units)])
    b, hidden, by_gate, by_up = hidden_units(b_own, by_hidden, w["w_gate"], w["w_up"])
    (by_h,) = reduce("by_states", 3, as_they_are, [by_gate, by_up], across, [h, dy], 1, finish_back, 80)
    on_x, on_y, on_chip = 4, 2, 1
    from_x, from_y, own2 = hop(by_h, on_x), hop(by_h, on_y), hop(by_h, on_chip)
    by_w = {"w_gate": mm("td,tu->du", b, by_gate), "w_up": mm("td,tu->du", b, by_up)}
    from_x, from_y, hidden, by_w = lax.optimization_barrier((from_x, from_y, hidden, by_w))
    far = [hop(from_y[:HALF], on_x), hop(from_x[HALF:], on_y)]
    x2, y2 = hop(from_x, on_chip), hop(from_y, on_chip)
    by_w["w_down"] = mm("tu,td->ud", hidden, all_dy)
    *far, by_w["w_down"] = lax.optimization_barrier((*far, by_w["w_down"]))
    pieces = [by_h, own2, from_x, x2, from_y, y2, *far, *(hop(t, on_chip) for t in far)]
    all_h, by_out, delta = by_heads(pieces, w["wo"], heads)
    by_q, by_k, by_v = attend_bwd(q, k, v, by_out, lse, delta, cos, sin)
    by_x, *rest = reduce("by_input", 4, heads_and_two, [by_q, by_k, by_v], [w["wq"], w["wk"], w["wv"]], [x, by_h], 1, finish_back, 60,
                         [fill_by_wo, fill_by_rest], [heads, all_h, a, by_q, by_k, by_v], [w[name].shape for name in ("wo", "wq", "wk", "wv")])
    by_w.update(zip(("wo", "wq", "wk", "wv"), rest))
    return by_x, by_w


def solution(mesh):
    def step(x, dy, *weights):
        by_x, by_w = layer(x[0], dy[0], dict(zip(NAMES, weights, strict=True)))
        return (by_x[None], *(by_w[name] for name in NAMES))

    states, by_columns, by_rows = P("dp", "tp", None), P(None, "tp"), P("tp", None)
    weights = (by_columns, by_columns, by_columns, by_rows, by_columns, by_columns, by_rows)
    own = tuple(P("dp", "tp") if spec == by_columns else P(("dp", "tp"), None) for spec in weights)
    return jax.shard_map(step, mesh=mesh, in_specs=(states, states, *weights), out_specs=(states, *own), check_vma=False)
```
